32 devices in a mesh: fsdp: 8 (over y, x, core), seq: 4 (over z).
Axes of the slice: x: 2, y: 2, z: 4, core: 2. Of those that a mesh axis runs over, the one named last changes fastest.
Arguments:
- layer_input: bfloat16 [8, 512, 4096], P('fsdp', 'seq'), may hold values from -6 to 6
- dt_weight: bfloat16 [4096, 64], P('fsdp'), may hold values from -0.09375 to 0.09375
- dt_bias: float32 [64], replicated, may hold values from -2 to -0.5
- decay_rate: float32 [64], replicated, may hold values from 0.0005 to 0.25
- ssm_input: bfloat16 [8, 512, 2048], P('fsdp', 'seq'), may hold values from -6 to 6
- in_basis: bfloat16 [8, 512, 512], P('fsdp', 'seq'), may hold values from -0.59765625 to 0.59765625
- out_basis: bfloat16 [8, 512, 512], P('fsdp', 'seq'), may hold values from -0.59765625 to 0.59765625
- out_cotangent: bfloat16 [8, 512, 2048], P('fsdp', 'seq'), may hold values from -6 to 6
Outputs:
- grad_input: bfloat16 [8, 512, 2048], P('fsdp', 'seq')
- grad_in_basis: bfloat16 [8, 512, 512], P('fsdp', 'seq')
- grad_out_basis: bfloat16 [8, 512, 512], P('fsdp', 'seq')
- grad_dt_weight: float32 [4096, 64], P('fsdp')
The draws below stay inside these ranges and needn't reach their ends.
All inputs are finite; a program needn't handle non-finite values.
Results may differ from the reference program's by a relative error of at most 0.011.
Values may be sent and summed in bfloat16 or wider, within the bound.
A program may use at most 64 MiB of HBM per device.

```python
import math
import jax
import jax.numpy as jnp
from jax import lax

D = 4096
HEADS = 64
HEAD_DIM = 32
GROUPS = 4
STATE = 128
TOK_DEV = 128
SEQLEN = 512
BATCH = 8
N_SEQ = 4


def raised(values, key, source, target, parts, factor):
    owner, partner = [(jnp.arange(values.shape[dim]) // (values.shape[dim] // parts)).reshape([-1 if axis == dim else 1 for axis in range(values.ndim)]) for dim in (source, target)]
    chosen = jax.random.permutation(key, parts)[partner]
    strong = (owner == chosen) | (owner == (partner + parts // 2) % parts)
    return jnp.where(strong, factor * values, values)


def level_of(rng, extent, split, low, largest):
    factor_of = 1.0
    for dim, shards_of in split:
        heights = jax.random.uniform(jax.random.fold_in(jax.random.fold_in(rng, 6), dim), (shards_of,), jnp.float32, low / len(split), largest / len(split))
        factor_of = factor_of * jnp.repeat(jnp.exp(heights), extent[dim] // shards_of).reshape((-1,) + (1,) * (len(extent) - 1 - dim))
    return factor_of


def bell_draw(key, extent, scale, reach, cuts=(), dtype=jnp.bfloat16):
    entries = jax.random.normal(key, extent, jnp.float32) * scale
    if len(cuts) > 0:
        entries = level_of(key, extent, cuts, -0.22, 0.18) * entries
    return jnp.clip(entries, min=-reach, max=reach).astype(dtype)


def gaussian_with(own_key, shape, scale, most, shards, heavy, held_as=jnp.bfloat16):
    array = scale * jax.random.normal(own_key, shape, jnp.float32)
    if shards:
        array = array * level_of(own_key, shape, shards, -0.22, 0.18)
    return jnp.clip(raised(array, jax.random.fold_in(own_key, 3), *heavy), -most, most).astype(held_as)


def setup_inputs(seed: int = 0) -> dict:
    streams_of = jax.random.split(jax.random.key(seed), 9)
    layer_input = gaussian_with(streams_of[0], (BATCH, SEQLEN, D), 1.0, 6.0, ((0, 8), (1, 4)), (0, 2, 8, 2.0))
    dt_weight = bell_draw(streams_of[1], (D, HEADS), D ** -0.5, 0.09375, ((0, 8),))
    dt_bias = jnp.clip(jax.random.uniform(streams_of[2], (HEADS,), jnp.float32, -2.0, -0.5), -2.0, -0.5)
    decay_rate = jnp.clip(jnp.exp(jax.random.uniform(streams_of[3], (HEADS,), jnp.float32, math.log(0.0005), math.log(0.25))), 0.0005, 0.25)
    ssm_input = bell_draw(streams_of[4], (BATCH, SEQLEN, HEADS * HEAD_DIM), 1.0, 6.0, ((0, 8), (1, 4)))
    in_basis = bell_draw(streams_of[5], (BATCH, SEQLEN, GROUPS * STATE), 0.09, 0.59765625, ((0, 8), (1, 4)))
    out_basis = bell_draw(streams_of[6], (BATCH, SEQLEN, GROUPS * STATE), 0.09, 0.59765625, ((0, 8), (1, 4)))
    out_cotangent = bell_draw(streams_of[7], (BATCH, SEQLEN, HEADS * HEAD_DIM), 1.0, 6.0, ((0, 8), (1, 4)))
    return {"layer_input": layer_input, "dt_weight": dt_weight, "dt_bias": dt_bias, "decay_rate": decay_rate, "ssm_input": ssm_input, "in_basis": in_basis, "out_basis": out_basis, "out_cotangent": out_cotangent}


HIGH = lax.Precision.HIGHEST

def block_step(state, pieces):
    logdecay, step_size, inputs, basis_in, basis_out = pieces
    cumulative = jnp.cumsum(logdecay, axis=0)
    final = cumulative[-1]
    rows_first = cumulative.T
    spread = rows_first[:, :, None] - rows_first[:, None, :]
    position = jnp.arange(logdecay.shape[0])
    lower = position[:, None] >= position[None, :]
    decay_mat = jnp.where(lower, jnp.exp(jnp.where(lower, spread, 0.0)), 0.0)
    intersection = jnp.einsum('thn,shn->hts', basis_out, basis_in, precision=HIGH)
    weighted = decay_mat * intersection
    inner = jnp.einsum('hts,sh,shp->thp', weighted, step_size, inputs, precision=HIGH)
    from_state = jnp.exp(cumulative)[:, :, None] * jnp.einsum('hpn,thn->thp', state, basis_out, precision=HIGH)
    tail = jnp.exp(final[None, :] - cumulative) * step_size
    new_state = jnp.exp(final)[:, None, None] * state + jnp.einsum('sh,shp,shn->hpn', tail, inputs, basis_in, precision=HIGH)
    return (new_state, inner + from_state)

def forward(weight, inputs, basis_in, basis_out, tokens, dt_bias, decay_rate):
    raw = jnp.dot(tokens, weight, precision=HIGH) + dt_bias
    step_size = jax.nn.softplus(raw)
    logdecay = -decay_rate * step_size
    per_group = HEADS // GROUPS
    inputs_h = inputs.reshape(N_SEQ, TOK_DEV, HEADS, HEAD_DIM)
    bin_h = jnp.repeat(basis_in.reshape(N_SEQ, TOK_DEV, GROUPS, STATE), per_group, axis=2)
    bout_h = jnp.repeat(basis_out.reshape(N_SEQ, TOK_DEV, GROUPS, STATE), per_group, axis=2)
    start = jnp.zeros((HEADS, HEAD_DIM, STATE), jnp.float32)
    pieces = (logdecay.reshape(N_SEQ, TOK_DEV, HEADS), step_size.reshape(N_SEQ, TOK_DEV, HEADS), inputs_h, bin_h, bout_h)
    _, outputs = lax.scan(block_step, start, pieces)
    return outputs.reshape(N_SEQ * TOK_DEV, HEADS * HEAD_DIM)

def reference(layer_input, dt_weight, dt_bias, decay_rate, ssm_input, in_basis, out_basis, out_cotangent):
    weight = dt_weight.astype(jnp.float32)

    def one_sequence(total, row):
        tokens, inputs, basis_in, basis_out, upstream = row
        tokens = tokens.astype(jnp.float32)

        def local(wmat, xval, bval, cval):
            return forward(wmat, xval, bval, cval, tokens, dt_bias, decay_rate)
        _, pull = jax.vjp(local, weight, inputs.astype(jnp.float32), basis_in.astype(jnp.float32), basis_out.astype(jnp.float32))
        grad_w, grad_x, grad_b, grad_c = pull(upstream.astype(jnp.float32))
        return (total + grad_w, (grad_x.astype(jnp.bfloat16), grad_b.astype(jnp.bfloat16), grad_c.astype(jnp.bfloat16)))
    start = jnp.zeros((D, HEADS), jnp.float32)
    total, (grad_x, grad_b, grad_c) = lax.scan(one_sequence, start, (layer_input, ssm_input, in_basis, out_basis, out_cotangent))
    return (grad_x, grad_b, grad_c, total)
```

```python
import functools

import jax
import jax.numpy as jnp
from jax import lax
from jax.experimental import pallas as pl
from jax.experimental.pallas import tpu as pltpu
from jax.sharding import PartitionSpec as P

STATE = 128
F32 = jnp.float32
BF16 = jnp.bfloat16
MESH = pl.DeviceIdType.MESH
HIGH = lax.Precision.HIGHEST


def dot(a, b, ca=1, cb=0, precision=None):
    return lax.dot_general(
        a, b, (((ca,), (cb,)), ((), ())), precision=precision, preferred_element_type=F32
    )


def halves(value, axis):
    high = value.astype(BF16)
    low = (value - high.astype(F32)).astype(BF16)
    return jnp.concatenate([high, low], axis=axis)


def iota(shape, dim):
    return lax.broadcasted_iota(jnp.int32, shape, dim)


QUARTER = 128


def kernel(
    nf,
    ns,
    tokens_hbm,
    weight_hbm,
    bias_hbm,
    rate_hbm,
    x_hbm,
    b_hbm,
    c_hbm,
    dy_hbm,
    out_x,
    out_b,
    out_c,
    out_w,
    tokens,
    bias,
    rate_row,
    x,
    b_in,
    c_out,
    dy,
    in_sem,
    own_sem,
    gathered,
    gathered_x,
    gathered_r,
    bias_t,
    rate_t,
    raw_t,
    cum_t,
    step_t,
    block_t,
    cum_g,
    step_g,
    decay_g,
    meet_g,
    spread_s,
    spread_st,
    state_loc,
    grad_loc,
    xs_g,
    ds_g,
    entry,
    later,
    send_f,
    send_b,
    through,
    joint,
    grad_b,
    grad_c,
    acc_b,
    acc_c,
    col_t,
    xt_t,
    xc_t,
    ent_t,
    z_early,
    z_last,
    ag_ssem,
    ag_rsem,
    x_ssem,
    x_rsem,
    r_ssem,
    r_rsem,
    f_ssem,
    f_rsem,
    b_ssem,
    b_rsem,
    z_ssem,
    z_rsem,
):
    f = lax.axis_index("fsdp")
    z = lax.axis_index("seq")
    length = tokens.shape[0]
    heads, rows = weight_hbm.shape
    groups = b_in.shape[1] // STATE
    per = heads // groups
    wide = x.shape[1] // groups
    size = wide // per
    quarters = wide // QUARTER
    few = QUARTER // size
    bits = nf.bit_length() - 1
    last = groups - 1

    def partner(m):
        return f + sum(
            (1 - 2 * ((f // 2**j) % 2)) * 2**j for j in range(bits) if (m // 2**j) % 2
        )

    far_first = sorted(range(1, nf), key=lambda m: -bin(m // 2).count("1"))

    own_weight = pltpu.make_async_copy(weight_hbm, gathered.at[f], own_sem.at[0])
    own_weight.start()
    barrier = pltpu.get_barrier_semaphore()
    for m in far_first:
        pl.semaphore_signal(
            barrier, inc=1, device_id={"fsdp": partner(m)}, device_id_type=MESH
        )

    @pl.when(z < ns - 1)
    def _():
        pl.semaphore_signal(
            barrier, inc=1, device_id={"seq": z + 1}, device_id_type=MESH
        )

    @pl.when(z > 0)
    def _():
        pl.semaphore_signal(
            barrier, inc=1, device_id={"seq": z - 1}, device_id_type=MESH
        )

    loads = [
        pltpu.make_async_copy(source, target, in_sem.at[n])
        for n, (source, target) in enumerate(
            (
                (bias_hbm, bias),
                (rate_hbm, rate_row),
                (tokens_hbm, tokens),
                (x_hbm, x),
                (b_hbm, b_in),
                (dy_hbm, dy),
                (c_hbm, c_out),
            )
        )
    ]
    for load in loads:
        load.start()
    loads[0].wait()
    loads[1].wait()
    bias_t[...] = jnp.broadcast_to(bias[...], (length, heads)).T
    rate_t[...] = jnp.broadcast_to(rate_row[...], (length, heads)).T
    own_weight.wait()
    ends = (z > 0).astype(jnp.int32) + (z < ns - 1).astype(jnp.int32)
    pl.semaphore_wait(barrier, nf - 1 + ends)

    def span_of(g, width):
        start = g * width
        return pl.ds(start if isinstance(start, int) else pl.multiple_of(start, width), width)

    def weight_copy(g, m):
        part = gathered.at[f, span_of(g, per)]
        return pltpu.make_async_remote_copy(
            src_ref=part,
            dst_ref=part,
            send_sem=ag_ssem.at[g, m - 1],
            recv_sem=ag_rsem.at[g, m - 1],
            device_id={"fsdp": partner(m)},
            device_id_type=MESH,
        )

    def token_copy(m):
        return pltpu.make_async_remote_copy(
            src_ref=tokens.at[:, span_of(partner(m), rows)],
            dst_ref=gathered_x.at[span_of(f, length)],
            send_sem=x_ssem.at[m - 1],
            recv_sem=x_rsem.at[m - 1],
            device_id={"fsdp": partner(m)},
            device_id_type=MESH,
        )

    def raw_copy(g, m):
        part = gathered_r.at[f, span_of(g, per)]
        return pltpu.make_async_remote_copy(
            src_ref=part,
            dst_ref=part,
            send_sem=r_ssem.at[g, m - 1],
            recv_sem=r_rsem.at[g, m - 1],
            device_id={"fsdp": partner(m)},
            device_id_type=MESH,
        )

    for g in range(groups):
        for m in far_first:
            weight_copy(g, m).start()
    for load in loads[2:]:
        load.wait()
    own_tokens = pltpu.make_async_copy(
        tokens.at[:, span_of(f, rows)], gathered_x.at[span_of(f, length)], own_sem.at[1]
    )
    own_tokens.start()
    for m in far_first:
        token_copy(m).start()

    @pl.when(z == 0)
    def _():
        entry[...] = jnp.zeros_like(entry)

    @pl.when(z == ns - 1)
    def _():
        later[...] = jnp.zeros_like(later)

    spread_one = (iota((2 * per, wide), 0) % per == iota((2 * per, wide), 1) // size).astype(BF16)
    gather_one = (iota((per, wide), 0) == iota((per, wide), 1) // size).astype(BF16)

    def expand(value):
        return dot(halves(value, 1), spread_one)

    def head_sums(value):
        width = value.shape[1]
        ones = (iota((width // size, width), 0) == iota((width // size, width), 1) // size).astype(BF16)
        high = value.astype(BF16)
        low = (value - high.astype(F32)).astype(BF16)
        return dot(ones, high, 1, 1) + dot(ones, low, 1, 1)

    def strip(q, n=1):
        return slice(q * QUARTER, (q + n) * QUARTER)

    def forward_copy(g, q):
        return pltpu.make_async_remote_copy(
            src_ref=send_f.at[g, strip(q)],
            dst_ref=entry.at[g, strip(q)],
            send_sem=f_ssem.at[g, q],
            recv_sem=f_rsem.at[g, q],
            device_id={"seq": (z + 1) % ns},
            device_id_type=MESH,
        )

    def backward_copy(g, q):
        return pltpu.make_async_remote_copy(
            src_ref=send_b.at[g, strip(q)],
            dst_ref=later.at[g, strip(q)],
            send_sem=b_ssem.at[g, q],
            recv_sem=b_rsem.at[g, q],
            device_id={"seq": (z + ns - 1) % ns},
            device_id_type=MESH,
        )

    def prepare(g):
        for m in range(1, nf):
            weight_copy(g, m).wait_recv()
        mine = span_of(g, per)
        weight = jnp.concatenate([gathered[own, mine] for own in range(nf)], axis=1)
        rate = rate_t[mine]
        raw = bias_t[mine] + dot(weight, tokens[...], 1, 1)
        step = jnp.maximum(raw, 0.0) + jnp.log1p(jnp.exp(-jnp.abs(raw)))
        before = iota((length, length), 0) <= iota((length, length), 1)
        cum = dot(-rate * step, before.astype(F32), precision=HIGH)
        raw_t[mine] = raw
        cum_t[mine] = cum
        step_t[mine] = step
        final = cum[:, length - 1 : length]
        block = jnp.broadcast_to(jnp.exp(final), (per, STATE))
        block_t[mine] = block
        decay_g[g] = dot(spread_one, halves(block, 0), 0, 0)
        both = jnp.concatenate([cum, step], axis=0).T
        cum_c = both[:, :per]
        step_c = both[:, per:]
        cum_g[g] = cum_c
        step_g[g] = step_c
        scale = expand(step_c * jnp.exp(cum_c[length - 1 : length] - cum_c))
        spread_st[g] = scale
        b = b_in[:, span_of(g, STATE)]
        c = c_out[:, span_of(g, STATE)]
        xs = (x[:, span_of(g, wide)].astype(F32) * scale).astype(BF16)
        ds = (dy[:, span_of(g, wide)].astype(F32) * expand(jnp.exp(cum_c))).astype(BF16)
        xs_g[g] = xs
        ds_g[g] = ds
        state = dot(xs, b, 0, 0)
        grad = dot(ds, c, 0, 0)
        state_loc[g] = state
        grad_loc[g] = grad

        @pl.when(z == 0)
        def _():
            send_f[g] = state.astype(BF16)
            for q in range(quarters):
                forward_copy(g, q).start()

        @pl.when(z == ns - 1)
        def _():
            send_b[g] = grad.astype(BF16)
            for q in range(quarters):
                backward_copy(g, q).start()

        spread_s[g] = expand(step_c)
        meet_g[g] = dot(b, c, 1, 1)

    def chain_f(g, q):
        @pl.when(z > 0)
        def _():
            forward_copy(g, q).wait_recv()

        @pl.when(jnp.logical_and(z > 0, z < ns - 1))
        def _():
            s = strip(q)
            send_f[g, s] = (decay_g[g, s] * entry[g, s].astype(F32) + state_loc[g, s]).astype(BF16)
            forward_copy(g, q).start()

    def chain_b(g, q):
        @pl.when(z < ns - 1)
        def _():
            backward_copy(g, q).wait_recv()

        @pl.when(jnp.logical_and(z > 0, z < ns - 1))
        def _():
            s = strip(q)
            send_b[g, s] = (decay_g[g, s] * later[g, s].astype(F32) + grad_loc[g, s]).astype(BF16)
            backward_copy(g, q).start()

    def columns(g, q, n=1):
        return pl.ds(pl.multiple_of(g * wide + q * QUARTER, QUARTER), n * QUARTER)

    def heavy(g, q):
        x_q = x[:, columns(g, q)]
        dy_q = dy[:, columns(g, q)]
        meet = meet_g[g]
        upper = iota((length, length), 0) <= iota((length, length), 1)
        lanes = iota((length, QUARTER), 1)
        cum_r = cum_t[span_of(g, per)]
        cum_l = cum_g[g]
        step_l = step_g[g]
        total = jnp.zeros((length, length), F32) if q == 0 else joint[...]
        sums = []
        weights = []
        masked = []
        for j in range(few):
            k = q * few + j
            mine = lanes // size == j
            pair = dot(jnp.where(mine, x_q, jnp.zeros_like(x_q)), dy_q, 1, 1)
            spread = cum_r[k : k + 1] - cum_l[:, k : k + 1]
            decay = jnp.exp(jnp.where(upper, spread, -1e30))
            weights.append((decay * meet).astype(BF16))
            masked.append(jnp.where(mine, dy_q, jnp.zeros_like(dy_q)))
            scaled = decay * pair * step_l[:, k : k + 1]
            total = total + scaled
            sums.append(jnp.sum(scaled * meet, axis=0, keepdims=True))
        passed = dot(jnp.concatenate(weights, axis=1), jnp.concatenate(masked, axis=0))
        through[g, :, strip(q)] = spread_s[g, :, strip(q)] * passed
        col_t[g, q] = jnp.concatenate(sums, axis=0)
        xt_t[g, q] = head_sums(x_q.astype(F32) * passed)
        if q < quarters - 1:
            joint[...] = total
        else:
            total = total.astype(BF16)
            grad_b[g] = dot(total, c_out[:, span_of(g, STATE)])
            grad_c[g] = dot(total, b_in[:, span_of(g, STATE)], 0, 0)

    def finish_f(g, q, n):
        c = c_out[:, span_of(g, STATE)]
        state = entry[g, strip(q, n)]
        ds = ds_g[g, :, strip(q, n)]
        sums = head_sums(ds.astype(F32) * dot(c, state, 1, 1))
        for i in range(n):
            ent_t[g, q + i] = sums[i * few : (i + 1) * few]
        value = dot(ds, state)
        if q > 0:
            value = value + acc_c[...]
        if q + n < quarters:
            acc_c[...] = value
        else:
            out_c[:, span_of(g, STATE)] = (grad_c[g] + value).astype(BF16)

    def finish_b(g, q, n):
        b = b_in[:, span_of(g, STATE)]
        grad = later[g, strip(q, n)]
        carried = dot(b, grad, 1, 1)
        sums = head_sums(x[:, columns(g, q, n)].astype(F32) * carried)
        for i in range(n):
            xc_t[g, q + i] = sums[i * few : (i + 1) * few]
        out_x[:, columns(g, q, n)] = (
            through[g, :, strip(q, n)] + spread_st[g, :, strip(q, n)] * carried
        ).astype(BF16)
        value = dot(xs_g[g, :, strip(q, n)], grad)
        if q > 0:
            value = value + acc_b[...]
        if q + n < quarters:
            acc_b[...] = value
        else:
            out_b[:, span_of(g, STATE)] = (grad_b[g] + value).astype(BF16)

    def post(g):
        mine = span_of(g, per)
        crossing = dot(
            gather_one, (entry[g].astype(F32) * later[g].astype(F32)).astype(BF16)
        )
        cum = cum_t[mine]
        step = step_t[mine]
        rate = rate_t[mine]

        def stacked(parts):
            return jnp.concatenate([parts[g, q] for q in range(quarters)], axis=0)

        xt = stacked(xt_t)
        tail_xc = jnp.exp(cum[:, length - 1 : length] - cum) * stacked(xc_t)
        leaving = step * tail_xc
        grad_cum = stacked(col_t) - step * xt + stacked(ent_t) - leaving
        closing = block_t[mine, :1] * jnp.sum(crossing, axis=1, keepdims=True) + jnp.sum(
            leaving, axis=1, keepdims=True
        )
        after = (iota((length, length), 0) >= iota((length, length), 1)).astype(F32)
        grad_log = dot(grad_cum, after, precision=HIGH) + closing
        grad_raw = (xt + tail_xc - rate * grad_log) * jax.nn.sigmoid(raw_t[mine])
        gathered_r[f, mine] = grad_raw.astype(BF16)
        for m in far_first:
            raw_copy(g, m).start()

    def within(g):
        return jnp.logical_and(g >= 0, g < groups)

    furthest = jnp.maximum(z, ns - 1 - z)

    def slot_step(tau, carry):
        gf = tau - z
        gb = tau - (ns - 1 - z)
        for q in range(quarters):
            pl.when(within(gf))(lambda: chain_f(gf, q))
            pl.when(within(gb))(lambda: chain_b(gb, q))
            if q == 0:
                pl.when(tau + 1 < groups)(lambda: prepare(tau + 1))
            pl.when(within(tau))(lambda: heavy(tau, q))
            if (q + 1) % FINISH == 0:
                at = q + 1 - FINISH
                pl.when(within(gf))(lambda: finish_f(gf, at, FINISH))
                pl.when(within(gb))(lambda: finish_b(gb, at, FINISH))
        pl.when(within(tau - furthest))(lambda: post(tau - furthest))
        return carry

    lax.fori_loop(-1, groups + ns - 1, slot_step, 0)

    def product(first, count):
        raws = jnp.concatenate(
            [gathered_r[own, first * per : (first + count) * per] for own in range(nf)], axis=1
        )
        return dot(raws, gathered_x[...]).astype(BF16)

    def exchange(target, n):
        copies = []
        for d in range(1, ns):
            copy = pltpu.make_async_remote_copy(
                src_ref=target.at[z],
                dst_ref=target.at[z],
                send_sem=z_ssem.at[n, d - 1],
                recv_sem=z_rsem.at[n, d - 1],
                device_id={"seq": (z + d) % ns},
                device_id_type=MESH,
            )
            copy.start()
            copies.append(copy)
        return copies

    own_tokens.wait()
    for m in range(1, nf):
        token_copy(m).wait_recv()
    for g in range(last):
        for m in range(1, nf):
            raw_copy(g, m).wait_recv()
    z_early[z] = product(0, last)
    early = exchange(z_early, 0)
    for m in range(1, nf):
        raw_copy(last, m).wait_recv()
    z_last[z] = product(last, 1)
    late = exchange(z_last, 1)
    for copies, source, place in (
        (early, z_early, slice(0, last * per)),
        (late, z_last, slice(last * per, heads)),
    ):
        for copy in copies:
            copy.wait()
        summed = source[0].astype(F32)
        for k in range(1, ns):
            summed = summed + source[k].astype(F32)
        out_w[place] = summed

    for m in range(1, nf):
        token_copy(m).wait_send()
        for g in range(groups):
            weight_copy(g, m).wait_send()
            raw_copy(g, m).wait_send()

    @pl.when(z < ns - 1)
    def _():
        for g in range(groups):
            for q in range(quarters):
                forward_copy(g, q).wait_send()

    @pl.when(z > 0)
    def _():
        for g in range(groups):
            for q in range(quarters):
                backward_copy(g, q).wait_send()


def ship(*refs):
    sems = refs[-1]
    count = len(refs) // 2
    copies = [
        pltpu.make_async_copy(refs[n], refs[count + n], sems.at[n]) for n in range(count)
    ]
    for copy in copies:
        copy.start()
    for copy in copies:
        copy.wait()


def general_kernel(
    nf,
    ns,
    tokens_hbm,
    weight_t,
    bias,
    rate_row,
    x_hbm,
    b_hbm,
    c_hbm,
    dy_hbm,
    x_out,
    b_out,
    c_out_hbm,
    out_w,
    tokens,
    x,
    b_in,
    c_out,
    dy,
    out_x,
    out_b,
    out_c,
    in_sem,
    out_sem,
    gathered,
    raw_t,
    cum_t,
    step_t,
    block_t,
    cum_g,
    step_g,
    tail_g,
    lead_g,
    state_loc,
    grad_loc,
    xs_g,
    ds_g,
    entry,
    later,
    send_f,
    send_b,
    through,
    grad_b,
    grad_c,
    col_t,
    xt_t,
    xc_t,
    ent_t,
    total,
    rs_send,
    rs_recv,
    z_recv,
    ag_ssem,
    ag_rsem,
    f_ssem,
    f_rsem,
    b_ssem,
    b_rsem,
    rs_ssem,
    rs_rsem,
    z_ssem,
    z_rsem,
):
    f = lax.axis_index("fsdp")
    z = lax.axis_index("seq")
    length = tokens.shape[0]
    heads, rows = weight_t.shape
    groups = b_in.shape[1] // STATE
    per = heads // groups
    wide = x.shape[1] // groups
    size = wide // per
    bits = nf.bit_length() - 1
    part_heads = heads // 2
    chunk = wide // 2
    loads = [
        pltpu.make_async_copy(source, target, in_sem.at[n])
        for n, (source, target) in enumerate(
            (
                (tokens_hbm, tokens),
                (x_hbm, x),
                (dy_hbm, dy),
                (b_hbm, b_in),
                (c_hbm, c_out),
            )
        )
    ]
    for load in loads:
        load.start()
    orders = (list(reversed(range(bits))), list(range(1, bits)) + [0])

    def slot_of(index, order):
        return sum(((index // 2**b) % 2) * 2**i for i, b in enumerate(order))

    def partner(j):
        return f + (1 - 2 * ((f // 2**j) % 2)) * 2**j

    barrier = pltpu.get_barrier_semaphore()
    for j in range(bits):
        pl.semaphore_signal(
            barrier, inc=1, device_id={"fsdp": partner(j)}, device_id_type=MESH
        )
    for d in range(1, ns):
        pl.semaphore_signal(
            barrier, inc=1, device_id={"seq": (z + d) % ns}, device_id_type=MESH
        )
    pl.semaphore_wait(barrier, bits + ns - 1)

    slots = [slot_of(f, order) for order in orders]
    for h in range(2):
        gathered[h, slots[h]] = weight_t[h * part_heads : (h + 1) * part_heads]
    for i in range(bits):
        copies = []
        for h in range(2):
            part = gathered.at[h, pl.ds((slots[h] // 2**i) * 2**i, 2**i)]
            copy = pltpu.make_async_remote_copy(
                src_ref=part,
                dst_ref=part,
                send_sem=ag_ssem.at[h, i],
                recv_sem=ag_rsem.at[h, i],
                device_id={"fsdp": partner(orders[h][i])},
                device_id_type=MESH,
            )
            copy.start()
            copies.append(copy)
        if i == bits - 1:
            for load in loads:
                load.wait()
        for copy in copies:
            copy.wait()

    raw = jnp.broadcast_to(bias[...], (length, heads)).T
    rate = jnp.broadcast_to(rate_row[...], (length, heads)).T
    for own in range(nf):
        weight = jnp.concatenate(
            [gathered[h, slot_of(own, orders[h])] for h in range(2)], axis=0
        )
        raw = raw + dot(weight, tokens[:, own * rows : (own + 1) * rows], 1, 1)
    step = jnp.maximum(raw, 0.0) + jnp.log1p(jnp.exp(-jnp.abs(raw)))
    before = iota((length, length), 0) <= iota((length, length), 1)
    cum = dot(-rate * step, before.astype(F32), precision=HIGH)
    raw_t[...] = raw
    cum_t[...] = cum
    step_t[...] = step
    final = cum[:, length - 1 : length]
    block_t[...] = jnp.broadcast_to(jnp.exp(final), (heads, STATE))
    both = jnp.concatenate([cum, step], axis=0).T
    cum_c = both[:, :heads]
    step_c = both[:, heads:]
    tail_c = jnp.exp(cum_c[length - 1 : length] - cum_c)
    lead_c = jnp.exp(cum_c)
    for g in range(groups):
        span = slice(g * per, (g + 1) * per)
        cum_g[g] = cum_c[:, span]
        step_g[g] = step_c[:, span]
        tail_g[g] = tail_c[:, span]
        lead_g[g] = lead_c[:, span]

    spread_one = (iota((2 * per, wide), 0) % per == iota((2 * per, wide), 1) // size).astype(BF16)
    gather_one = (iota((per, wide), 0) == iota((per, wide), 1) // size).astype(BF16)

    def expand(value):
        return dot(halves(value, 1), spread_one)

    def head_sums(value):
        high = value.astype(BF16)
        low = (value - high.astype(F32)).astype(BF16)
        return dot(gather_one, high, 1, 1) + dot(gather_one, low, 1, 1)

    def span_of(g, width):
        return pl.ds(pl.multiple_of(g * width, width), width)

    @pl.when(z == 0)
    def _():
        entry[...] = jnp.zeros_like(entry)

    @pl.when(z == ns - 1)
    def _():
        later[...] = jnp.zeros_like(later)

    spread_half = (
        iota((per, chunk), 0) % (per // 2) == iota((per, chunk), 1) // size
    ).astype(BF16)

    def piece(g):
        return g // 2, pl.ds(pl.multiple_of((g % 2) * chunk, chunk), chunk)

    def forward_copy(g):
        return pltpu.make_async_remote_copy(
            src_ref=send_f.at[piece(g)],
            dst_ref=entry.at[piece(g)],
            send_sem=f_ssem.at[g],
            recv_sem=f_rsem.at[g],
            device_id={"seq": (z + 1) % ns},
            device_id_type=MESH,
        )

    def backward_copy(g):
        return pltpu.make_async_remote_copy(
            src_ref=send_b.at[piece(g)],
            dst_ref=later.at[piece(g)],
            send_sem=b_ssem.at[g],
            recv_sem=b_rsem.at[g],
            device_id={"seq": (z + ns - 1) % ns},
            device_id_type=MESH,
        )

    def local(g):
        xs = (x[:, span_of(g, wide)].astype(F32) * expand(step_g[g] * tail_g[g])).astype(BF16)
        ds = (dy[:, span_of(g, wide)].astype(F32) * expand(lead_g[g])).astype(BF16)
        xs_g[g] = xs
        ds_g[g] = ds
        state_loc[g] = dot(xs, b_in[:, span_of(g, STATE)], 0, 0)
        grad_loc[g] = dot(ds, c_out[:, span_of(g, STATE)], 0, 0)

    def decay_rows(g):
        return dot(spread_half, halves(block_t[span_of(g, per // 2)], 0), 0, 0)

    def chain_f(g):
        @pl.when(z > 0)
        def _():
            forward_copy(g).wait_recv()

        @pl.when(z < ns - 1)
        def _():
            p = piece(g)
            send_f[p] = (decay_rows(g) * entry[p].astype(F32) + state_loc[p]).astype(BF16)
            forward_copy(g).start()

    def chain_b(g):
        @pl.when(z < ns - 1)
        def _():
            backward_copy(g).wait_recv()

        @pl.when(z > 0)
        def _():
            p = piece(g)
            send_b[p] = (decay_rows(g) * later[p].astype(F32) + grad_loc[p]).astype(BF16)
            backward_copy(g).start()

    def heavy(g):
        inputs = x[:, span_of(g, wide)]
        upstream = dy[:, span_of(g, wide)]
        b = b_in[:, span_of(g, STATE)]
        c = c_out[:, span_of(g, STATE)]
        meet = dot(b, c, 1, 1)
        upper = iota((length, length), 0) <= iota((length, length), 1)
        lanes = iota((length, 128), 1)
        cum_r = cum_t[span_of(g, per)]
        cum_l = cum_g[g]
        step_l = step_g[g]
        joint = jnp.zeros((length, length), F32)
        sums = []
        pieces = []
        for q in range(wide // 128):
            x_q = inputs[:, q * 128 : (q + 1) * 128]
            dy_q = upstream[:, q * 128 : (q + 1) * 128]
            weights = []
            masked = []
            for j in range(128 // size):
                k = q * (128 // size) + j
                mine = lanes // size == j
                pair = dot(jnp.where(mine, x_q, jnp.zeros_like(x_q)), dy_q, 1, 1)
                spread = cum_r[k : k + 1] - cum_l[:, k : k + 1]
                decay = jnp.exp(jnp.where(upper, spread, -1e30))
                weights.append((decay * meet).astype(BF16))
                masked.append(jnp.where(mine, dy_q, jnp.zeros_like(dy_q)))
                scaled = decay * pair * step_l[:, k : k + 1]
                joint = joint + scaled
                sums.append(jnp.sum(scaled * meet, axis=0, keepdims=True))
            pieces.append(
                dot(jnp.concatenate(weights, axis=1), jnp.concatenate(masked, axis=0))
            )
        passed = jnp.concatenate(pieces, axis=1)
        through[g] = passed
        col_t[span_of(g, per)] = jnp.concatenate(sums, axis=0)
        xt_t[span_of(g, per)] = head_sums(inputs.astype(F32) * passed)
        joint = joint.astype(BF16)
        grad_b[g] = dot(joint, c)
        grad_c[g] = dot(joint, b, 0, 0)

    def finish_f(g):
        c = c_out[:, span_of(g, STATE)]
        read = dot(c, entry[g], 1, 1)
        ent_t[span_of(g, per)] = head_sums(ds_g[g].astype(F32) * read)
        out_c[:, span_of(g, STATE)] = (grad_c[g] + dot(ds_g[g], entry[g])).astype(BF16)

    def finish_b(g):
        b = b_in[:, span_of(g, STATE)]
        carried = dot(b, later[g], 1, 1)
        xc_t[span_of(g, per)] = head_sums(x[:, span_of(g, wide)].astype(F32) * carried)
        inner = through[g] + expand(tail_g[g]) * carried
        out_x[:, span_of(g, wide)] = (expand(step_g[g]) * inner).astype(BF16)
        out_b[:, span_of(g, STATE)] = (grad_b[g] + dot(xs_g[g], later[g])).astype(BF16)

    def within(g):
        return jnp.logical_and(g >= 0, g < groups)

    def slot_step(tau, carry):
        gf = tau - z
        gb = tau - (ns - 1 - z)
        pl.when(tau < groups)(lambda: local(tau))
        pl.when(within(gf))(lambda: chain_f(2 * gf))
        pl.when(within(gb))(lambda: chain_b(2 * gb))
        pl.when(tau < groups)(lambda: heavy(tau))
        pl.when(within(gf))(lambda: chain_f(2 * gf + 1))
        pl.when(within(gb))(lambda: chain_b(2 * gb + 1))
        pl.when(within(gf))(lambda: finish_f(gf))
        pl.when(within(gb))(lambda: finish_b(gb))
        return carry

    lax.fori_loop(0, groups + ns - 1, slot_step, 0)
    stores = [
        pltpu.make_async_copy(source, target, out_sem.at[n])
        for n, (source, target) in enumerate(
            ((out_x, x_out), (out_b, b_out), (out_c, c_out_hbm))
        )
    ]
    for store in stores:
        store.start()

    crossing = jnp.concatenate(
        [
            dot(gather_one, (entry[g].astype(F32) * later[g].astype(F32)).astype(BF16))
            for g in range(groups)
        ],
        axis=0,
    )
    cum = cum_t[...]
    step = step_t[...]
    raw = raw_t[...]
    tail = jnp.exp(cum[:, length - 1 : length] - cum)
    xt = xt_t[...]
    tail_xc = tail * xc_t[...]
    leaving = step * tail_xc
    grad_cum = col_t[...] - step * xt + ent_t[...] - leaving
    closing = block_t[:, :1] * jnp.sum(crossing, axis=1, keepdims=True) + jnp.sum(
        leaving, axis=1, keepdims=True
    )
    after = (iota((length, length), 0) >= iota((length, length), 1)).astype(F32)
    grad_log = dot(grad_cum, after, precision=HIGH) + closing
    grad_raw = (xt + tail_xc - rate * grad_log) * jax.nn.sigmoid(raw)
    grad_raw = grad_raw.astype(BF16)

    bases = [0, 0]
    count = nf
    early = rows % 128 == 0

    def product(own, target, place, offset):
        columns = pl.ds(pl.multiple_of(own * rows, 128), rows) if early else slice(
            own * rows, (own + 1) * rows
        )
        block = dot(grad_raw, tokens[:, columns])
        for h in range(2):
            target[h, offset + place[h]] = block[
                h * part_heads : (h + 1) * part_heads
            ].astype(target.dtype)

    for j in range(bits):
        half = count // 2
        sent = pl.ds(nf - count, half)
        if j == 0 and early:
            bit = f % 2
            for i in range(half):
                place = [slot_of(2 * i, order) for order in orders]
                product(2 * i + (1 - bit), rs_send, place, 0)
        elif j == 0:
            for own in range(nf):
                product(own, total, [slot_of(own, order) for order in orders], 0)
        copies = []
        for h in range(2):
            b = orders[h][bits - 1 - j]
            bit_h = (f // 2**b) % 2
            if j > 0 or not early:
                rs_send[h, sent] = total[
                    h, pl.ds(bases[h] + (1 - bit_h) * half, half)
                ].astype(BF16)
            copy = pltpu.make_async_remote_copy(
                src_ref=rs_send.at[h, sent],
                dst_ref=rs_recv.at[h, sent],
                send_sem=rs_ssem.at[h, j],
                recv_sem=rs_rsem.at[h, j],
                device_id={"fsdp": partner(b)},
                device_id_type=MESH,
            )
            copy.start()
            copies.append(copy)
            bases[h] = bases[h] + bit_h * half
        if j == 0 and early:
            for i in range(half):
                place = [slot_of(2 * i, order) for order in orders]
                product(2 * i + bit, total, place, bit * half)
        for h in range(2):
            copies[h].wait()
            total[h, pl.ds(bases[h], half)] += rs_recv[h, sent].astype(F32)
        count = half

    z_recv[z] = jnp.concatenate([total[h, bases[h]] for h in range(2)], axis=0).astype(BF16)
    copies = []
    for d in range(1, ns):
        copy = pltpu.make_async_remote_copy(
            src_ref=z_recv.at[z],
            dst_ref=z_recv.at[z],
            send_sem=z_ssem.at[d - 1],
            recv_sem=z_rsem.at[d - 1],
            device_id={"seq": (z + d) % ns},
            device_id_type=MESH,
        )
        copy.start()
        copies.append(copy)
    for copy in copies:
        copy.wait()
    summed = z_recv[0].astype(F32)
    for k in range(1, ns):
        summed = summed + z_recv[k].astype(F32)
    out_w[...] = summed

    @pl.when(z < ns - 1)
    def _():
        for g in range(2 * groups):
            forward_copy(g).wait_send()

    @pl.when(z > 0)
    def _():
        for g in range(2 * groups):
            backward_copy(g).wait_send()

    for store in stores:
        store.wait()


def general_body(
    layer_input, dt_weight, dt_bias, decay_rate, ssm_input, in_basis, out_basis, out_cotangent
):
    nf, ns = lax.axis_size("fsdp"), lax.axis_size("seq")
    length = layer_input.shape[1]
    rows, heads = dt_weight.shape
    groups = in_basis.shape[2] // STATE
    per = heads // groups
    full = ssm_input.shape[2]
    wide = full // groups
    bits = nf.bit_length() - 1
    tall = (groups, wide, STATE)
    dma = pltpu.SemaphoreType.DMA
    v = pltpu.VMEM
    scratch = [
        v((length, layer_input.shape[2]), BF16),
        v((length, full), BF16),
        v((length, groups * STATE), BF16),
        v((length, groups * STATE), BF16),
        v((length, full), BF16),
        v((length, full), BF16),
        v((length, groups * STATE), BF16),
        v((length, groups * STATE), BF16),
        dma((5,)),
        dma((3,)),
        v((2, nf, heads // 2, rows), BF16),
        v((heads, length), F32),
        v((heads, length), F32),
        v((heads, length), F32),
        v((heads, STATE), F32),
        v((groups, length, per), F32),
        v((groups, length, per), F32),
        v((groups, length, per), F32),
        v((groups, length, per), F32),
        v(tall, F32),
        v(tall, F32),
        v((groups, length, wide), BF16),
        v((groups, length, wide), BF16),
        v(tall, BF16),
        v(tall, BF16),
        v(tall, BF16),
        v(tall, BF16),
        v((groups, length, wide), F32),
        v((groups, length, STATE), F32),
        v((groups, length, STATE), F32),
        v((heads, length), F32),
        v((heads, length), F32),
        v((heads, length), F32),
        v((heads, length), F32),
        v((2, nf, heads // 2, rows), F32),
        v((2, nf, heads // 2, rows), BF16),
        v((2, nf, heads // 2, rows), BF16),
        v((ns, heads, rows), BF16),
        dma((2, bits)),
        dma((2, bits)),
        dma((2 * groups,)),
        dma((2 * groups,)),
        dma((2 * groups,)),
        dma((2 * groups,)),
        dma((2, bits)),
        dma((2, bits)),
        dma((ns - 1,)),
        dma((ns - 1,)),
    ]
    anywhere = pl.BlockSpec(memory_space=pl.ANY)
    inside = pl.BlockSpec(memory_space=pltpu.VMEM)
    out_x, out_b, out_c, out_w = pl.pallas_call(
        functools.partial(general_kernel, nf, ns),
        out_shape=(
            jax.ShapeDtypeStruct((length, full), BF16),
            jax.ShapeDtypeStruct((length, groups * STATE), BF16),
            jax.ShapeDtypeStruct((length, groups * STATE), BF16),
            jax.ShapeDtypeStruct((heads, rows), F32),
        ),
        in_specs=[anywhere] + [inside] * 3 + [anywhere] * 4,
        out_specs=[anywhere] * 3 + [inside],
        scratch_shapes=scratch,
        compiler_params=pltpu.CompilerParams(
            collective_id=0, has_side_effects=True, vmem_limit_bytes=60 * 1024 * 1024
        ),
    )(
        layer_input[0],
        dt_weight.T,
        dt_bias[None],
        decay_rate[None],
        ssm_input[0],
        in_basis[0],
        out_basis[0],
        out_cotangent[0],
    )
    return (out_x[None], out_b[None], out_c[None], out_w.T)


FINISH = 2


def body(
    layer_input, dt_weight, dt_bias, decay_rate, ssm_input, in_basis, out_basis, out_cotangent
):
    nf, ns = lax.axis_size("fsdp"), lax.axis_size("seq")
    length = layer_input.shape[1]
    rows, heads = dt_weight.shape
    groups = in_basis.shape[2] // STATE
    per = heads // groups
    full = ssm_input.shape[2]
    wide = full // groups
    size = wide // per
    quarters = wide // QUARTER
    few = QUARTER // size
    tall = (groups, wide, STATE)
    flat = (groups, length, wide)
    dma = pltpu.SemaphoreType.DMA
    v = pltpu.VMEM
    scratch = [
        v((length, layer_input.shape[2]), BF16),
        v((1, heads), F32),
        v((1, heads), F32),
        v((length, full), BF16),
        v((length, groups * STATE), BF16),
        v((length, groups * STATE), BF16),
        v((length, full), BF16),
        dma((7,)),
        dma((2,)),
        v((nf, heads, rows), BF16),
        v((nf * length, rows), BF16),
        v((nf, heads, length), BF16),
        v((heads, length), F32),
        v((heads, length), F32),
        v((heads, length), F32),
        v((heads, length), F32),
        v((heads, length), F32),
        v((heads, STATE), F32),
        v((groups, length, per), F32),
        v((groups, length, per), F32),
        v(tall, F32),
        v((groups, length, length), F32),
        v(flat, F32),
        v(flat, F32),
        v(tall, F32),
        v(tall, F32),
        v(flat, BF16),
        v(flat, BF16),
        v(tall, BF16),
        v(tall, BF16),
        v(tall, BF16),
        v(tall, BF16),
        v(flat, F32),
        v((length, length), F32),
        v((groups, length, STATE), F32),
        v((groups, length, STATE), F32),
        v((length, STATE), F32),
        v((length, STATE), F32),
        v((groups, quarters, few, length), F32),
        v((groups, quarters, few, length), F32),
        v((groups, quarters, few, length), F32),
        v((groups, quarters, few, length), F32),
        v((ns, heads - per, rows), BF16),
        v((ns, per, rows), BF16),
        dma((groups, nf - 1)),
        dma((groups, nf - 1)),
        dma((nf - 1,)),
        dma((nf - 1,)),
        dma((groups, nf - 1)),
        dma((groups, nf - 1)),
        dma((groups, quarters)),
        dma((groups, quarters)),
        dma((groups, quarters)),
        dma((groups, quarters)),
        dma((2, ns - 1)),
        dma((2, ns - 1)),
    ]
    inside = pl.BlockSpec(memory_space=pltpu.VMEM)
    outside = pl.BlockSpec(memory_space=pltpu.HBM)
    operands = (
        layer_input[0],
        dt_weight.T,
        dt_bias[None],
        decay_rate[None],
        ssm_input[0],
        in_basis[0],
        out_basis[0],
        out_cotangent[0],
    )
    results = pl.pallas_call(
        functools.partial(kernel, nf, ns),
        out_shape=(
            jax.ShapeDtypeStruct((length, full), BF16),
            jax.ShapeDtypeStruct((length, groups * STATE), BF16),
            jax.ShapeDtypeStruct((length, groups * STATE), BF16),
            jax.ShapeDtypeStruct((heads, rows), F32),
        ),
        in_specs=[outside] * len(operands),
        out_specs=[inside] * 4,
        scratch_shapes=scratch,
        compiler_params=pltpu.CompilerParams(
            collective_id=0, has_side_effects=True, vmem_limit_bytes=40 * 1024 * 1024
        ),
    )(*[pltpu.with_memory_space_constraint(a, pltpu.HBM) for a in operands])
    anywhere = pl.BlockSpec(memory_space=pl.ANY)
    out_x, out_b, out_c, out_w = pl.pallas_call(
        ship,
        out_shape=[jax.ShapeDtypeStruct(r.shape, r.dtype) for r in results],
        in_specs=[anywhere] * 4,
        out_specs=[anywhere] * 4,
        scratch_shapes=[dma((4,))],
        compiler_params=pltpu.CompilerParams(vmem_limit_bytes=1024 * 1024),
    )(*results)
    return (out_x[None], out_b[None], out_c[None], out_w.T)


def solution(mesh):
    blocks = P("fsdp", "seq", None)
    rows = P("fsdp", None)

    def local(*args):
        nf = lax.axis_size("fsdp")
        shard = args[1].shape[0]
        lanes = args[4].shape[2] * STATE // args[5].shape[2]
        fits = shard % 128 == 0 and nf & (nf - 1) == 0 and lanes % QUARTER == 0
        return (body if fits else general_body)(*args)

    return jax.shard_map(
        local,
        mesh=mesh,
        in_specs=(blocks, rows, P(), P(), blocks, blocks, blocks, blocks),
        out_specs=(blocks, blocks, blocks, rows),
        check_vma=False,
    )
```

```python
import functools

import jax
import jax.numpy as jnp
from jax import lax
from jax.experimental import pallas as pl
from jax.experimental.pallas import tpu as pltpu
from jax.sharding import PartitionSpec as P

STATE = 128
F32 = jnp.float32
BF16 = jnp.bfloat16
MESH = pl.DeviceIdType.MESH
HIGH = lax.Precision.HIGHEST


def dot(a, b, ca=1, cb=0, precision=None):
    return lax.dot_general(
        a, b, (((ca,), (cb,)), ((), ())), precision=precision, preferred_element_type=F32
    )


def halves(value, axis):
    high = value.astype(BF16)
    low = (value - high.astype(F32)).astype(BF16)
    return jnp.concatenate([high, low], axis=axis)


def iota(shape, dim):
    return lax.broadcasted_iota(jnp.int32, shape, dim)


QUARTER = 128
PIECE = 64
AHEAD = 2
LOG2_E = 1.4426950408889634


def kernel(
    nf,
    ns,
    tokens_hbm,
    weight_hbm,
    bias_hbm,
    rate_hbm,
    x_hbm,
    b_hbm,
    c_hbm,
    dy_hbm,
    out_x,
    out_b,
    out_c,
    out_w,
    tokens,
    bias,
    rate_row,
    x,
    b_in,
    c_out,
    dy,
    in_sem,
    own_sem,
    gathered,
    gathered_x,
    gathered_r,
    bias_t,
    rate_t,
    raw_t,
    cum_t,
    step_t,
    block_t,
    cum_g,
    step_g,
    decay_g,
    meet_g,
    spread_s,
    spread_st,
    state_loc,
    grad_loc,
    xs_g,
    ds_g,
    entry,
    later,
    send_f,
    send_b,
    through,
    joint,
    grad_b,
    grad_c,
    col_t,
    xt_t,
    xc_t,
    ent_t,
    z_recv,
    ag_ssem,
    ag_rsem,
    x_ssem,
    x_rsem,
    r_ssem,
    r_rsem,
    f_ssem,
    f_rsem,
    b_ssem,
    b_rsem,
    z_ssem,
    z_rsem,
):
    f = lax.axis_index("fsdp")
    z = lax.axis_index("seq")
    length = tokens.shape[0]
    heads, rows = weight_hbm.shape
    groups = b_in.shape[1] // STATE
    per = heads // groups
    wide = x.shape[1] // groups
    size = wide // per
    quarters = wide // QUARTER
    parts = wide // PIECE
    few = QUARTER // size
    bits = nf.bit_length() - 1
    last = groups - 1

    def partner(m):
        return f + sum(
            (1 - 2 * ((f // 2**j) % 2)) * 2**j for j in range(bits) if (m // 2**j) % 2
        )

    near_first = sorted(range(1, nf), key=lambda m: bin(m // 2).count("1"))
    far_first = near_first[::-1]

    own_weight = pltpu.make_async_copy(weight_hbm, gathered.at[f], own_sem.at[0])
    own_weight.start()
    barrier = pltpu.get_barrier_semaphore()
    for m in far_first:
        pl.semaphore_signal(
            barrier, inc=1, device_id={"fsdp": partner(m)}, device_id_type=MESH
        )

    @pl.when(z < ns - 1)
    def _():
        pl.semaphore_signal(
            barrier, inc=1, device_id={"seq": z + 1}, device_id_type=MESH
        )

    @pl.when(z > 0)
    def _():
        pl.semaphore_signal(
            barrier, inc=1, device_id={"seq": z - 1}, device_id_type=MESH
        )

    loads = [
        pltpu.make_async_copy(source, target, in_sem.at[n])
        for n, (source, target) in enumerate(
            (
                (bias_hbm, bias),
                (rate_hbm, rate_row),
                (tokens_hbm, tokens),
                (x_hbm, x),
                (b_hbm, b_in),
                (dy_hbm, dy),
                (c_hbm, c_out),
            )
        )
    ]
    for load in loads:
        load.start()
    loads[0].wait()
    loads[1].wait()
    bias_t[...] = jnp.broadcast_to(bias[...], (length, heads)).T
    rate_t[...] = jnp.broadcast_to(rate_row[...], (length, heads)).T
    own_weight.wait()
    ends = (z > 0).astype(jnp.int32) + (z < ns - 1).astype(jnp.int32)
    pl.semaphore_wait(barrier, nf - 1 + ends)

    def span_of(g, width):
        start = g * width
        return pl.ds(start if isinstance(start, int) else pl.multiple_of(start, width), width)

    def weight_copy(g, m):
        part = gathered.at[f, span_of(g, per)]
        return pltpu.make_async_remote_copy(
            src_ref=part,
            dst_ref=part,
            send_sem=ag_ssem.at[g, m - 1],
            recv_sem=ag_rsem.at[g, m - 1],
            device_id={"fsdp": partner(m)},
            device_id_type=MESH,
        )

    def token_copy(m):
        return pltpu.make_async_remote_copy(
            src_ref=tokens.at[:, span_of(partner(m), rows)],
            dst_ref=gathered_x.at[span_of(f, length)],
            send_sem=x_ssem.at[m - 1],
            recv_sem=x_rsem.at[m - 1],
            device_id={"fsdp": partner(m)},
            device_id_type=MESH,
        )

    def raw_copy(g, m):
        part = gathered_r.at[f, span_of(g, per)]
        return pltpu.make_async_remote_copy(
            src_ref=part,
            dst_ref=part,
            send_sem=r_ssem.at[g, m - 1],
            recv_sem=r_rsem.at[g, m - 1],
            device_id={"fsdp": partner(m)},
            device_id_type=MESH,
        )

    for m in far_first:
        weight_copy(0, m).start()
    for load in loads[2:]:
        load.wait()
    own_tokens = pltpu.make_async_copy(
        tokens.at[:, span_of(f, rows)], gathered_x.at[span_of(f, length)], own_sem.at[1]
    )
    own_tokens.start()

    @pl.when(z == 0)
    def _():
        entry[...] = jnp.zeros_like(entry)

    @pl.when(z == ns - 1)
    def _():
        later[...] = jnp.zeros_like(later)

    spread_one = (iota((2 * per, wide), 0) % per == iota((2 * per, wide), 1) // size).astype(BF16)
    gather_one = (iota((per, wide), 0) == iota((per, wide), 1) // size).astype(BF16)

    def expand(value):
        return dot(halves(value, 1), spread_one)

    def head_sums(value):
        width = value.shape[1]
        ones = (iota((width // size, width), 0) == iota((width // size, width), 1) // size).astype(BF16)
        high = value.astype(BF16)
        low = (value - high.astype(F32)).astype(BF16)
        return dot(ones, high, 1, 1) + dot(ones, low, 1, 1)

    def part(p):
        return slice(p * PIECE, (p + 1) * PIECE)

    def strip(q):
        return slice(q * QUARTER, (q + 1) * QUARTER)

    def forward_copy(g, p):
        return pltpu.make_async_remote_copy(
            src_ref=send_f.at[g, part(p)],
            dst_ref=entry.at[g, part(p)],
            send_sem=f_ssem.at[g, p],
            recv_sem=f_rsem.at[g, p],
            device_id={"seq": (z + 1) % ns},
            device_id_type=MESH,
        )

    def backward_copy(g, p):
        return pltpu.make_async_remote_copy(
            src_ref=send_b.at[g, part(p)],
            dst_ref=later.at[g, part(p)],
            send_sem=b_ssem.at[g, p],
            recv_sem=b_rsem.at[g, p],
            device_id={"seq": (z + ns - 1) % ns},
            device_id_type=MESH,
        )

    def thirds(value, axis):
        high = value.astype(BF16)
        rest = value - high.astype(F32)
        middle = rest.astype(BF16)
        low = (rest - middle.astype(F32)).astype(BF16)
        return jnp.concatenate([high, middle, low], axis=axis)

    def steps(g, product):
        mine = span_of(g, per)
        raw = bias_t[mine] + product
        step = jnp.maximum(raw, 0.0) + jnp.log1p(jnp.exp(-jnp.abs(raw)))
        before = iota((3 * length, length), 0) % length <= iota((3 * length, length), 1)
        cum = dot(thirds(-LOG2_E * rate_t[mine] * step, 1), before.astype(BF16))
        both = jnp.concatenate([cum, step], axis=0).T
        cum_c = both[:, :per]
        step_c = both[:, per:]
        cum_g[g] = cum_c
        step_g[g] = step_c
        raw_t[mine] = raw
        cum_t[mine] = cum
        step_t[mine] = step
        block_t[mine] = jnp.broadcast_to(jnp.exp2(cum[:, length - 1 : length]), (per, STATE))
        return cum_c, step_c

    def gather(g):
        for m in far_first:
            weight_copy(g, m).start()

    def prepare_first():
        mine = span_of(0, per)
        product = dot(gathered[f, mine], tokens[:, span_of(f, rows)], 1, 1)
        for n, m in enumerate(near_first):
            weight_copy(0, m).wait_recv()
            if n == 0:
                gather(1)
            elif n == nf // 2:
                gather(2)
            own = partner(m)
            product = product + dot(gathered[own, mine], tokens[:, span_of(own, rows)], 1, 1)
        for g in range(3, groups):
            gather(g)
        return steps(0, product)

    def prepare(g):
        for m in near_first:
            weight_copy(g, m).wait_recv()
        mine = span_of(g, per)
        weight = jnp.concatenate([gathered[own, mine] for own in range(nf)], axis=1)
        steps(g, dot(weight, tokens[...], 1, 1))

        @pl.when(g == 2)
        def _():
            for m in far_first:
                token_copy(m).start()

    def local(g, cum_c, step_c, opening=False):
        scale = expand(step_c * jnp.exp2(cum_c[length - 1 : length] - cum_c))
        b = b_in[:, span_of(g, STATE)]
        c = c_out[:, span_of(g, STATE)]
        xs = (x[:, span_of(g, wide)].astype(F32) * scale).astype(BF16)
        ds = (dy[:, span_of(g, wide)].astype(F32) * expand(jnp.exp2(cum_c))).astype(BF16)
        state = dot(xs, b, 0, 0)
        grad = dot(ds, c, 0, 0)
        spread_st[g] = scale
        xs_g[g] = xs
        ds_g[g] = ds

        @pl.when(z == 0)
        def _():
            send_f[g] = state.astype(BF16)
            if opening:
                for p in range(AHEAD):
                    forward_copy(g, p).start()

        @pl.when(z == ns - 1)
        def _():
            send_b[g] = grad.astype(BF16)
            if opening:
                for p in range(AHEAD):
                    backward_copy(g, p).start()

        state_loc[g] = state
        grad_loc[g] = grad
        decay_g[g] = dot(spread_one, halves(block_t[span_of(g, per)], 0), 0, 0)
        spread_s[g] = expand(step_c)
        meet_g[g] = dot(b, c, 1, 1)

    def chain_f(g, p):
        @pl.when(z > 0)
        def _():
            forward_copy(g, p).wait_recv()

        @pl.when(jnp.logical_and(z > 0, z < ns - 1))
        def _():
            s = part(p)
            send_f[g, s] = (decay_g[g, s] * entry[g, s].astype(F32) + state_loc[g, s]).astype(BF16)

        @pl.when(z < ns - 1 if p >= AHEAD else (z < ns - 1) & ((z > 0) | (g > 0)))
        def _():
            forward_copy(g, p).start()

    def chain_b(g, p):
        @pl.when(z < ns - 1)
        def _():
            backward_copy(g, p).wait_recv()

        @pl.when(jnp.logical_and(z > 0, z < ns - 1))
        def _():
            s = part(p)
            send_b[g, s] = (decay_g[g, s] * later[g, s].astype(F32) + grad_loc[g, s]).astype(BF16)

        @pl.when(z > 0 if p >= AHEAD else (z > 0) & ((z < ns - 1) | (g > 0)))
        def _():
            backward_copy(g, p).start()

    def columns(g, q):
        return pl.ds(pl.multiple_of(g * wide + q * QUARTER, QUARTER), QUARTER)

    def heavy(g, q0, n):
        meet = meet_g[g]
        upper = iota((length, length), 0) <= iota((length, length), 1)
        lanes = iota((length, QUARTER), 1)
        cum_r = cum_t[span_of(g, per)]
        cum_l = cum_g[g]
        step_l = step_g[g]
        total = jnp.zeros((length, length), F32) if q0 == 0 else joint[...]
        for q in range(q0, q0 + n):
            x_q = x[:, columns(g, q)]
            dy_q = dy[:, columns(g, q)]
            sums = []
            weights = []
            masked = []
            split = [jnp.where(lanes // size == j, x_q, jnp.zeros_like(x_q)) for j in range(few)]
            pairs = dot(jnp.concatenate(split, axis=0), dy_q, 1, 1)
            for j in range(few):
                k = q * few + j
                mine = lanes // size == j
                pair = pairs[j * length : (j + 1) * length]
                spread = cum_r[k : k + 1] - cum_l[:, k : k + 1]
                decay = jnp.exp2(jnp.where(upper, spread, -1e30))
                weights.append((decay * meet).astype(BF16))
                masked.append(jnp.where(mine, dy_q, jnp.zeros_like(dy_q)))
                scaled = decay * pair * step_l[:, k : k + 1]
                total = total + scaled
                sums.append(jnp.sum(scaled * meet, axis=0, keepdims=True))
            passed = dot(jnp.concatenate(weights, axis=1), jnp.concatenate(masked, axis=0))
            through[g, :, strip(q)] = spread_s[g, :, strip(q)] * passed
            col_t[g, q] = jnp.concatenate(sums, axis=0)
            xt_t[g, q] = head_sums(x_q.astype(F32) * passed)
        if q0 + n < quarters:
            joint[...] = total
        else:
            total = total.astype(BF16)
            grad_b[g] = dot(total, c_out[:, span_of(g, STATE)])
            grad_c[g] = dot(total, b_in[:, span_of(g, STATE)], 0, 0)

    def sums_f(g):
        @pl.when(z == 0)
        def _():
            ent_t[span_of(g, per)] = jnp.zeros((per, length), F32)

        @pl.when(z > 0)
        def _():
            read = dot(c_out[:, span_of(g, STATE)], entry[g], 1, 1)
            ent_t[span_of(g, per)] = head_sums(ds_g[g].astype(F32) * read)

    def sums_b(g):
        @pl.when(z == ns - 1)
        def _():
            xc_t[span_of(g, per)] = jnp.zeros((per, length), F32)

        @pl.when(z < ns - 1)
        def _():
            carried = dot(b_in[:, span_of(g, STATE)], later[g], 1, 1)
            xc_t[span_of(g, per)] = head_sums(x[:, span_of(g, wide)].astype(F32) * carried)

    def results_f(g):
        columns = span_of(g, STATE)

        @pl.when(z == 0)
        def _():
            out_c[:, columns] = grad_c[g].astype(BF16)

        @pl.when(z > 0)
        def _():
            out_c[:, columns] = (grad_c[g] + dot(ds_g[g], entry[g])).astype(BF16)

    def results_b(g):
        columns = span_of(g, STATE)
        channels = span_of(g, wide)

        @pl.when(z == ns - 1)
        def _():
            out_x[:, channels] = through[g].astype(BF16)
            out_b[:, columns] = grad_b[g].astype(BF16)

        @pl.when(z < ns - 1)
        def _():
            grad = later[g]
            carried = dot(b_in[:, columns], grad, 1, 1)
            out_x[:, channels] = (through[g] + spread_st[g] * carried).astype(BF16)
            out_b[:, columns] = (grad_b[g] + dot(xs_g[g], grad)).astype(BF16)

    def finish_f(g):
        columns = span_of(g, STATE)

        @pl.when(z == 0)
        def _():
            ent_t[span_of(g, per)] = jnp.zeros((per, length), F32)
            out_c[:, columns] = grad_c[g].astype(BF16)

        @pl.when(z > 0)
        def _():
            state = entry[g]
            ds = ds_g[g]
            read = dot(c_out[:, columns], state, 1, 1)
            ent_t[span_of(g, per)] = head_sums(ds.astype(F32) * read)
            out_c[:, columns] = (grad_c[g] + dot(ds, state)).astype(BF16)

    def finish_b(g):
        columns = span_of(g, STATE)
        channels = span_of(g, wide)

        @pl.when(z == ns - 1)
        def _():
            xc_t[span_of(g, per)] = jnp.zeros((per, length), F32)
            out_x[:, channels] = through[g].astype(BF16)
            out_b[:, columns] = grad_b[g].astype(BF16)

        @pl.when(z < ns - 1)
        def _():
            grad = later[g]
            carried = dot(b_in[:, columns], grad, 1, 1)
            xc_t[span_of(g, per)] = head_sums(x[:, channels].astype(F32) * carried)
            out_x[:, channels] = (through[g] + spread_st[g] * carried).astype(BF16)
            out_b[:, columns] = (grad_b[g] + dot(xs_g[g], grad)).astype(BF16)

    def post(g):
        mine = span_of(g, per)
        crossing = dot(
            gather_one, (entry[g].astype(F32) * later[g].astype(F32)).astype(BF16)
        )
        cum = cum_t[mine]
        step = step_t[mine]
        rate = rate_t[mine]

        def stacked(parts):
            return jnp.concatenate([parts[g, q] for q in range(quarters)], axis=0)

        xt = stacked(xt_t)
        tail_xc = jnp.exp2(cum[:, length - 1 : length] - cum) * xc_t[mine]
        leaving = step * tail_xc
        grad_cum = stacked(col_t) - step * xt + ent_t[mine] - leaving
        closing = block_t[mine, :1] * jnp.sum(crossing, axis=1, keepdims=True) + jnp.sum(
            leaving, axis=1, keepdims=True
        )
        after = iota((3 * length, length), 0) % length >= iota((3 * length, length), 1)
        grad_log = dot(thirds(grad_cum, 1), after.astype(BF16)) + closing
        grad_raw = (xt + tail_xc - rate * grad_log) * jax.nn.sigmoid(raw_t[mine])
        gathered_r[f, mine] = grad_raw.astype(BF16)
        for m in far_first:
            raw_copy(g, m).start()

    def within(g):
        return jnp.logical_and(g >= 0, g < groups)

    furthest = jnp.maximum(z, ns - 1 - z)

    def slot_step(tau, carry):
        gf = tau - z
        gb = tau - (ns - 1 - z)
        whole = tau - furthest
        half = quarters // 2
        both = jnp.logical_and
        lag = tau <= groups + 1
        now = tau > groups
        early = tau + 1 < groups
        edge = furthest == ns - 1
        first = jnp.where(edge | (tau < 2), tau, jnp.where(tau == 2, -1, tau - 1))
        second = jnp.where(edge | (tau < 1), tau, jnp.where(tau == 1, -1, tau - 1))
        stride = parts // 4
        for p in range(parts):
            pl.when(within(gf))(lambda: chain_f(gf, p))
            pl.when(within(gb))(lambda: chain_b(gb, p))
            if p == stride - 1:
                pl.when(early)(lambda: prepare(tau + 1))
                pl.when(within(gf - 1) & lag & (tau + 1 >= groups))(lambda: finish_f(gf - 1))
            elif p == 2 * stride - 1:
                pl.when(within(first))(lambda: heavy(first, 0, half))
                pl.when(within(gf - 1) & early)(lambda: finish_f(gf - 1))
            elif p == 3 * stride - 1:
                pl.when(early)(lambda: local(tau + 1, cum_g[tau + 1], step_g[tau + 1]))
                pl.when(both(within(gb - 1), lag))(lambda: finish_b(gb - 1))
                pl.when(both(within(whole - 1), lag))(lambda: post(whole - 1))
            elif p == 4 * stride - 1:
                pl.when(within(second))(lambda: heavy(second, half, quarters - half))
        pl.when(both(within(gf), now))(lambda: sums_f(gf))
        pl.when(both(within(gb), now))(lambda: sums_b(gb))
        pl.when(both(within(whole), now))(lambda: post(whole))
        pl.when(both(within(gf), now))(lambda: results_f(gf))
        pl.when(both(within(gb), now))(lambda: results_b(gb))
        return carry

    local(0, *prepare_first(), opening=True)
    lax.fori_loop(0, groups + ns - 1, slot_step, 0)

    def product(first, count):
        raws = jnp.concatenate(
            [gathered_r[own, first * per : (first + count) * per] for own in range(nf)], axis=1
        )
        return dot(raws, gathered_x[...]).astype(BF16)

    own_tokens.wait()
    for m in range(1, nf):
        token_copy(m).wait_recv()
    shares = []
    for n, (first, count) in enumerate(((0, groups - 2), (groups - 2, 1), (groups - 1, 1))):
        for g in range(first, first + count):
            for m in range(1, nf):
                raw_copy(g, m).wait_recv()
        place = slice(first * per, (first + count) * per)
        z_recv[z, place] = product(first, count)
        copies = []
        for d in range(1, ns):
            share = z_recv.at[z, place]
            copy = pltpu.make_async_remote_copy(
                src_ref=share,
                dst_ref=share,
                send_sem=z_ssem.at[n, d - 1],
                recv_sem=z_rsem.at[n, d - 1],
                device_id={"seq": (z + d) % ns},
                device_id_type=MESH,
            )
            copy.start()
            copies.append(copy)
        shares.append((place, copies))
    for m in range(1, nf):
        token_copy(m).wait_send()
        for g in range(groups):
            weight_copy(g, m).wait_send()
            raw_copy(g, m).wait_send()

    @pl.when(z < ns - 1)
    def _():
        for g in range(groups):
            for p in range(parts):
                forward_copy(g, p).wait_send()

    @pl.when(z > 0)
    def _():
        for g in range(groups):
            for p in range(parts):
                backward_copy(g, p).wait_send()

    for place, copies in shares:
        for copy in copies:
            copy.wait_recv()
        summed = z_recv[0, place].astype(F32)
        for k in range(1, ns):
            summed = summed + z_recv[k, place].astype(F32)
        out_w[place] = summed

    for _, copies in shares:
        for copy in copies:
            copy.wait_send()


def ship(*refs):
    sems = refs[-1]
    count = len(refs) // 2
    copies = [
        pltpu.make_async_copy(refs[n], refs[count + n], sems.at[n]) for n in range(count)
    ]
    for copy in copies:
        copy.start()
    for copy in copies:
        copy.wait()


def general_kernel(
    nf,
    ns,
    tokens_hbm,
    weight_t,
    bias,
    rate_row,
    x_hbm,
    b_hbm,
    c_hbm,
    dy_hbm,
    x_out,
    b_out,
    c_out_hbm,
    out_w,
    tokens,
    x,
    b_in,
    c_out,
    dy,
    out_x,
    out_b,
    out_c,
    in_sem,
    out_sem,
    gathered,
    raw_t,
    cum_t,
    step_t,
    block_t,
    cum_g,
    step_g,
    tail_g,
    lead_g,
    state_loc,
    grad_loc,
    xs_g,
    ds_g,
    entry,
    later,
    send_f,
    send_b,
    through,
    grad_b,
    grad_c,
    col_t,
    xt_t,
    xc_t,
    ent_t,
    total,
    rs_send,
    rs_recv,
    z_recv,
    ag_ssem,
    ag_rsem,
    f_ssem,
    f_rsem,
    b_ssem,
    b_rsem,
    rs_ssem,
    rs_rsem,
    z_ssem,
    z_rsem,
):
    f = lax.axis_index("fsdp")
    z = lax.axis_index("seq")
    length = tokens.shape[0]
    heads, rows = weight_t.shape
    groups = b_in.shape[1] // STATE
    per = heads // groups
    wide = x.shape[1] // groups
    size = wide // per
    bits = nf.bit_length() - 1
    part_heads = heads // 2
    chunk = wide // 2
    loads = [
        pltpu.make_async_copy(source, target, in_sem.at[n])
        for n, (source, target) in enumerate(
            (
                (tokens_hbm, tokens),
                (x_hbm, x),
                (dy_hbm, dy),
                (b_hbm, b_in),
                (c_hbm, c_out),
            )
        )
    ]
    for load in loads:
        load.start()
    orders = (list(reversed(range(bits))), list(range(1, bits)) + [0])

    def slot_of(index, order):
        return sum(((index // 2**b) % 2) * 2**i for i, b in enumerate(order))

    def partner(j):
        return f + (1 - 2 * ((f // 2**j) % 2)) * 2**j

    barrier = pltpu.get_barrier_semaphore()
    for j in range(bits):
        pl.semaphore_signal(
            barrier, inc=1, device_id={"fsdp": partner(j)}, device_id_type=MESH
        )
    for d in range(1, ns):
        pl.semaphore_signal(
            barrier, inc=1, device_id={"seq": (z + d) % ns}, device_id_type=MESH
        )
    pl.semaphore_wait(barrier, bits + ns - 1)

    slots = [slot_of(f, order) for order in orders]
    for h in range(2):
        gathered[h, slots[h]] = weight_t[h * part_heads : (h + 1) * part_heads]
    for i in range(bits):
        copies = []
        for h in range(2):
            part = gathered.at[h, pl.ds((slots[h] // 2**i) * 2**i, 2**i)]
            copy = pltpu.make_async_remote_copy(
                src_ref=part,
                dst_ref=part,
                send_sem=ag_ssem.at[h, i],
                recv_sem=ag_rsem.at[h, i],
                device_id={"fsdp": partner(orders[h][i])},
                device_id_type=MESH,
            )
            copy.start()
            copies.append(copy)
        if i == bits - 1:
            for load in loads:
                load.wait()
        for copy in copies:
            copy.wait()

    raw = jnp.broadcast_to(bias[...], (length, heads)).T
    rate = jnp.broadcast_to(rate_row[...], (length, heads)).T
    for own in range(nf):
        weight = jnp.concatenate(
            [gathered[h, slot_of(own, orders[h])] for h in range(2)], axis=0
        )
        raw = raw + dot(weight, tokens[:, own * rows : (own + 1) * rows], 1, 1)
    step = jnp.maximum(raw, 0.0) + jnp.log1p(jnp.exp(-jnp.abs(raw)))
    before = iota((length, length), 0) <= iota((length, length), 1)
    cum = dot(-rate * step, before.astype(F32), precision=HIGH)
    raw_t[...] = raw
    cum_t[...] = cum
    step_t[...] = step
    final = cum[:, length - 1 : length]
    block_t[...] = jnp.broadcast_to(jnp.exp(final), (heads, STATE))
    both = jnp.concatenate([cum, step], axis=0).T
    cum_c = both[:, :heads]
    step_c = both[:, heads:]
    tail_c = jnp.exp(cum_c[length - 1 : length] - cum_c)
    lead_c = jnp.exp(cum_c)
    for g in range(groups):
        span = slice(g * per, (g + 1) * per)
        cum_g[g] = cum_c[:, span]
        step_g[g] = step_c[:, span]
        tail_g[g] = tail_c[:, span]
        lead_g[g] = lead_c[:, span]

    spread_one = (iota((2 * per, wide), 0) % per == iota((2 * per, wide), 1) // size).astype(BF16)
    gather_one = (iota((per, wide), 0) == iota((per, wide), 1) // size).astype(BF16)

    def expand(value):
        return dot(halves(value, 1), spread_one)

    def head_sums(value):
        high = value.astype(BF16)
        low = (value - high.astype(F32)).astype(BF16)
        return dot(gather_one, high, 1, 1) + dot(gather_one, low, 1, 1)

    def span_of(g, width):
        return pl.ds(pl.multiple_of(g * width, width), width)

    @pl.when(z == 0)
    def _():
        entry[...] = jnp.zeros_like(entry)

    @pl.when(z == ns - 1)
    def _():
        later[...] = jnp.zeros_like(later)

    spread_half = (
        iota((per, chunk), 0) % (per // 2) == iota((per, chunk), 1) // size
    ).astype(BF16)

    def piece(g):
        return g // 2, pl.ds(pl.multiple_of((g % 2) * chunk, chunk), chunk)

    def forward_copy(g):
        return pltpu.make_async_remote_copy(
            src_ref=send_f.at[piece(g)],
            dst_ref=entry.at[piece(g)],
            send_sem=f_ssem.at[g],
            recv_sem=f_rsem.at[g],
            device_id={"seq": (z + 1) % ns},
            device_id_type=MESH,
        )

    def backward_copy(g):
        return pltpu.make_async_remote_copy(
            src_ref=send_b.at[piece(g)],
            dst_ref=later.at[piece(g)],
            send_sem=b_ssem.at[g],
            recv_sem=b_rsem.at[g],
            device_id={"seq": (z + ns - 1) % ns},
            device_id_type=MESH,
        )

    def local(g):
        xs = (x[:, span_of(g, wide)].astype(F32) * expand(step_g[g] * tail_g[g])).astype(BF16)
        ds = (dy[:, span_of(g, wide)].astype(F32) * expand(lead_g[g])).astype(BF16)
        xs_g[g] = xs
        ds_g[g] = ds
        state_loc[g] = dot(xs, b_in[:, span_of(g, STATE)], 0, 0)
        grad_loc[g] = dot(ds, c_out[:, span_of(g, STATE)], 0, 0)

    def decay_rows(g):
        return dot(spread_half, halves(block_t[span_of(g, per // 2)], 0), 0, 0)

    def chain_f(g):
        @pl.when(z > 0)
        def _():
            forward_copy(g).wait_recv()

        @pl.when(z < ns - 1)
        def _():
            p = piece(g)
            send_f[p] = (decay_rows(g) * entry[p].astype(F32) + state_loc[p]).astype(BF16)
            forward_copy(g).start()

    def chain_b(g):
        @pl.when(z < ns - 1)
        def _():
            backward_copy(g).wait_recv()

        @pl.when(z > 0)
        def _():
            p = piece(g)
            send_b[p] = (decay_rows(g) * later[p].astype(F32) + grad_loc[p]).astype(BF16)
            backward_copy(g).start()

    def heavy(g):
        inputs = x[:, span_of(g, wide)]
        upstream = dy[:, span_of(g, wide)]
        b = b_in[:, span_of(g, STATE)]
        c = c_out[:, span_of(g, STATE)]
        meet = dot(b, c, 1, 1)
        upper = iota((length, length), 0) <= iota((length, length), 1)
        lanes = iota((length, 128), 1)
        cum_r = cum_t[span_of(g, per)]
        cum_l = cum_g[g]
        step_l = step_g[g]
        joint = jnp.zeros((length, length), F32)
        sums = []
        pieces = []
        for q in range(wide // 128):
            x_q = inputs[:, q * 128 : (q + 1) * 128]
            dy_q = upstream[:, q * 128 : (q + 1) * 128]
            weights = []
            masked = []
            for j in range(128 // size):
                k = q * (128 // size) + j
                mine = lanes // size == j
                pair = dot(jnp.where(mine, x_q, jnp.zeros_like(x_q)), dy_q, 1, 1)
                spread = cum_r[k : k + 1] - cum_l[:, k : k + 1]
                decay = jnp.exp(jnp.where(upper, spread, -1e30))
                weights.append((decay * meet).astype(BF16))
                masked.append(jnp.where(mine, dy_q, jnp.zeros_like(dy_q)))
                scaled = decay * pair * step_l[:, k : k + 1]
                joint = joint + scaled
                sums.append(jnp.sum(scaled * meet, axis=0, keepdims=True))
            pieces.append(
                dot(jnp.concatenate(weights, axis=1), jnp.concatenate(masked, axis=0))
            )
        passed = jnp.concatenate(pieces, axis=1)
        through[g] = passed
        col_t[span_of(g, per)] = jnp.concatenate(sums, axis=0)
        xt_t[span_of(g, per)] = head_sums(inputs.astype(F32) * passed)
        joint = joint.astype(BF16)
        grad_b[g] = dot(joint, c)
        grad_c[g] = dot(joint, b, 0, 0)

    def finish_f(g):
        c = c_out[:, span_of(g, STATE)]
        read = dot(c, entry[g], 1, 1)
        ent_t[span_of(g, per)] = head_sums(ds_g[g].astype(F32) * read)
        out_c[:, span_of(g, STATE)] = (grad_c[g] + dot(ds_g[g], entry[g])).astype(BF16)

    def finish_b(g):
        b = b_in[:, span_of(g, STATE)]
        carried = dot(b, later[g], 1, 1)
        xc_t[span_of(g, per)] = head_sums(x[:, span_of(g, wide)].astype(F32) * carried)
        inner = through[g] + expand(tail_g[g]) * carried
        out_x[:, span_of(g, wide)] = (expand(step_g[g]) * inner).astype(BF16)
        out_b[:, span_of(g, STATE)] = (grad_b[g] + dot(xs_g[g], later[g])).astype(BF16)

    def within(g):
        return jnp.logical_and(g >= 0, g < groups)

    def slot_step(tau, carry):
        gf = tau - z
        gb = tau - (ns - 1 - z)
        pl.when(tau < groups)(lambda: local(tau))
        pl.when(within(gf))(lambda: chain_f(2 * gf))
        pl.when(within(gb))(lambda: chain_b(2 * gb))
        pl.when(tau < groups)(lambda: heavy(tau))
        pl.when(within(gf))(lambda: chain_f(2 * gf + 1))
        pl.when(within(gb))(lambda: chain_b(2 * gb + 1))
        pl.when(within(gf))(lambda: finish_f(gf))
        pl.when(within(gb))(lambda: finish_b(gb))
        return carry

    lax.fori_loop(0, groups + ns - 1, slot_step, 0)
    stores = [
        pltpu.make_async_copy(source, target, out_sem.at[n])
        for n, (source, target) in enumerate(
            ((out_x, x_out), (out_b, b_out), (out_c, c_out_hbm))
        )
    ]
    for store in stores:
        store.start()

    crossing = jnp.concatenate(
        [
            dot(gather_one, (entry[g].astype(F32) * later[g].astype(F32)).astype(BF16))
            for g in range(groups)
        ],
        axis=0,
    )
    cum = cum_t[...]
    step = step_t[...]
    raw = raw_t[...]
    tail = jnp.exp(cum[:, length - 1 : length] - cum)
    xt = xt_t[...]
    tail_xc = tail * xc_t[...]
    leaving = step * tail_xc
    grad_cum = col_t[...] - step * xt + ent_t[...] - leaving
    closing = block_t[:, :1] * jnp.sum(crossing, axis=1, keepdims=True) + jnp.sum(
        leaving, axis=1, keepdims=True
    )
    after = (iota((length, length), 0) >= iota((length, length), 1)).astype(F32)
    grad_log = dot(grad_cum, after, precision=HIGH) + closing
    grad_raw = (xt + tail_xc - rate * grad_log) * jax.nn.sigmoid(raw)
    grad_raw = grad_raw.astype(BF16)

    bases = [0, 0]
    count = nf
    early = rows % 128 == 0

    def product(own, target, place, offset):
        columns = pl.ds(pl.multiple_of(own * rows, 128), rows) if early else slice(
            own * rows, (own + 1) * rows
        )
        block = dot(grad_raw, tokens[:, columns])
        for h in range(2):
            target[h, offset + place[h]] = block[
                h * part_heads : (h + 1) * part_heads
            ].astype(target.dtype)

    for j in range(bits):
        half = count // 2
        sent = pl.ds(nf - count, half)
        if j == 0 and early:
            bit = f % 2
            for i in range(half):
                place = [slot_of(2 * i, order) for order in orders]
                product(2 * i + (1 - bit), rs_send, place, 0)
        elif j == 0:
            for own in range(nf):
                product(own, total, [slot_of(own, order) for order in orders], 0)
        copies = []
        for h in range(2):
            b = orders[h][bits - 1 - j]
            bit_h = (f // 2**b) % 2
            if j > 0 or not early:
                rs_send[h, sent] = total[
                    h, pl.ds(bases[h] + (1 - bit_h) * half, half)
                ].astype(BF16)
            copy = pltpu.make_async_remote_copy(
                src_ref=rs_send.at[h, sent],
                dst_ref=rs_recv.at[h, sent],
                send_sem=rs_ssem.at[h, j],
                recv_sem=rs_rsem.at[h, j],
                device_id={"fsdp": partner(b)},
                device_id_type=MESH,
            )
            copy.start()
            copies.append(copy)
            bases[h] = bases[h] + bit_h * half
        if j == 0 and early:
            for i in range(half):
                place = [slot_of(2 * i, order) for order in orders]
                product(2 * i + bit, total, place, bit * half)
        for h in range(2):
            copies[h].wait()
            total[h, pl.ds(bases[h], half)] += rs_recv[h, sent].astype(F32)
        count = half

    z_recv[z] = jnp.concatenate([total[h, bases[h]] for h in range(2)], axis=0).astype(BF16)
    copies = []
    for d in range(1, ns):
        copy = pltpu.make_async_remote_copy(
            src_ref=z_recv.at[z],
            dst_ref=z_recv.at[z],
            send_sem=z_ssem.at[d - 1],
            recv_sem=z_rsem.at[d - 1],
            device_id={"seq": (z + d) % ns},
            device_id_type=MESH,
        )
        copy.start()
        copies.append(copy)
    for copy in copies:
        copy.wait()
    summed = z_recv[0].astype(F32)
    for k in range(1, ns):
        summed = summed + z_recv[k].astype(F32)
    out_w[...] = summed

    @pl.when(z < ns - 1)
    def _():
        for g in range(2 * groups):
            forward_copy(g).wait_send()

    @pl.when(z > 0)
    def _():
        for g in range(2 * groups):
            backward_copy(g).wait_send()

    for store in stores:
        store.wait()


def general_body(
    layer_input, dt_weight, dt_bias, decay_rate, ssm_input, in_basis, out_basis, out_cotangent
):
    nf, ns = lax.axis_size("fsdp"), lax.axis_size("seq")
    length = layer_input.shape[1]
    rows, heads = dt_weight.shape
    groups = in_basis.shape[2] // STATE
    per = heads // groups
    full = ssm_input.shape[2]
    wide = full // groups
    bits = nf.bit_length() - 1
    tall = (groups, wide, STATE)
    dma = pltpu.SemaphoreType.DMA
    v = pltpu.VMEM
    scratch = [
        v((length, layer_input.shape[2]), BF16),
        v((length, full), BF16),
        v((length, groups * STATE), BF16),
        v((length, groups * STATE), BF16),
        v((length, full), BF16),
        v((length, full), BF16),
        v((length, groups * STATE), BF16),
        v((length, groups * STATE), BF16),
        dma((5,)),
        dma((3,)),
        v((2, nf, heads // 2, rows), BF16),
        v((heads, length), F32),
        v((heads, length), F32),
        v((heads, length), F32),
        v((heads, STATE), F32),
        v((groups, length, per), F32),
        v((groups, length, per), F32),
        v((groups, length, per), F32),
        v((groups, length, per), F32),
        v(tall, F32),
        v(tall, F32),
        v((groups, length, wide), BF16),
        v((groups, length, wide), BF16),
        v(tall, BF16),
        v(tall, BF16),
        v(tall, BF16),
        v(tall, BF16),
        v((groups, length, wide), F32),
        v((groups, length, STATE), F32),
        v((groups, length, STATE), F32),
        v((heads, length), F32),
        v((heads, length), F32),
        v((heads, length), F32),
        v((heads, length), F32),
        v((2, nf, heads // 2, rows), F32),
        v((2, nf, heads // 2, rows), BF16),
        v((2, nf, heads // 2, rows), BF16),
        v((ns, heads, rows), BF16),
        dma((2, bits)),
        dma((2, bits)),
        dma((2 * groups,)),
        dma((2 * groups,)),
        dma((2 * groups,)),
        dma((2 * groups,)),
        dma((2, bits)),
        dma((2, bits)),
        dma((ns - 1,)),
        dma((ns - 1,)),
    ]
    anywhere = pl.BlockSpec(memory_space=pl.ANY)
    inside = pl.BlockSpec(memory_space=pltpu.VMEM)
    out_x, out_b, out_c, out_w = pl.pallas_call(
        functools.partial(general_kernel, nf, ns),
        out_shape=(
            jax.ShapeDtypeStruct((length, full), BF16),
            jax.ShapeDtypeStruct((length, groups * STATE), BF16),
            jax.ShapeDtypeStruct((length, groups * STATE), BF16),
            jax.ShapeDtypeStruct((heads, rows), F32),
        ),
        in_specs=[anywhere] + [inside] * 3 + [anywhere] * 4,
        out_specs=[anywhere] * 3 + [inside],
        scratch_shapes=scratch,
        compiler_params=pltpu.CompilerParams(
            collective_id=0, has_side_effects=True, vmem_limit_bytes=60 * 1024 * 1024
        ),
    )(
        layer_input[0],
        dt_weight.T,
        dt_bias[None],
        decay_rate[None],
        ssm_input[0],
        in_basis[0],
        out_basis[0],
        out_cotangent[0],
    )
    return (out_x[None], out_b[None], out_c[None], out_w.T)


def body(
    layer_input, dt_weight, dt_bias, decay_rate, ssm_input, in_basis, out_basis, out_cotangent
):
    nf, ns = lax.axis_size("fsdp"), lax.axis_size("seq")
    length = layer_input.shape[1]
    rows, heads = dt_weight.shape
    groups = in_basis.shape[2] // STATE
    per = heads // groups
    full = ssm_input.shape[2]
    wide = full // groups
    size = wide // per
    quarters = wide // QUARTER
    parts = wide // PIECE
    few = QUARTER // size
    tall = (groups, wide, STATE)
    flat = (groups, length, wide)
    dma = pltpu.SemaphoreType.DMA
    v = pltpu.VMEM
    scratch = [
        v((length, layer_input.shape[2]), BF16),
        v((1, heads), F32),
        v((1, heads), F32),
        v((length, full), BF16),
        v((length, groups * STATE), BF16),
        v((length, groups * STATE), BF16),
        v((length, full), BF16),
        dma((7,)),
        dma((2,)),
        v((nf, heads, rows), BF16),
        v((nf * length, rows), BF16),
        v((nf, heads, length), BF16),
        v((heads, length), F32),
        v((heads, length), F32),
        v((heads, length), F32),
        v((heads, length), F32),
        v((heads, length), F32),
        v((heads, STATE), F32),
        v((groups, length, per), F32),
        v((groups, length, per), F32),
        v(tall, F32),
        v((groups, length, length), F32),
        v(flat, F32),
        v(flat, F32),
        v(tall, F32),
        v(tall, F32),
        v(flat, BF16),
        v(flat, BF16),
        v(tall, BF16),
        v(tall, BF16),
        v(tall, BF16),
        v(tall, BF16),
        v(flat, F32),
        v((length, length), F32),
        v((groups, length, STATE), F32),
        v((groups, length, STATE), F32),
        v((groups, quarters, few, length), F32),
        v((groups, quarters, few, length), F32),
        v((heads, length), F32),
        v((heads, length), F32),
        v((ns, heads, rows), BF16),
        dma((groups, nf - 1)),
        dma((groups, nf - 1)),
        dma((nf - 1,)),
        dma((nf - 1,)),
        dma((groups, nf - 1)),
        dma((groups, nf - 1)),
        dma((groups, parts)),
        dma((groups, parts)),
        dma((groups, parts)),
        dma((groups, parts)),
        dma((3, ns - 1)),
        dma((3, ns - 1)),
    ]
    inside = pl.BlockSpec(memory_space=pltpu.VMEM)
    outside = pl.BlockSpec(memory_space=pltpu.HBM)
    operands = (
        layer_input[0],
        dt_weight.T,
        dt_bias[None],
        decay_rate[None],
        ssm_input[0],
        in_basis[0],
        out_basis[0],
        out_cotangent[0],
    )
    results = pl.pallas_call(
        functools.partial(kernel, nf, ns),
        out_shape=(
            jax.ShapeDtypeStruct((length, full), BF16),
            jax.ShapeDtypeStruct((length, groups * STATE), BF16),
            jax.ShapeDtypeStruct((length, groups * STATE), BF16),
            jax.ShapeDtypeStruct((heads, rows), F32),
        ),
        in_specs=[outside] * len(operands),
        out_specs=[inside] * 4,
        scratch_shapes=scratch,
        compiler_params=pltpu.CompilerParams(
            collective_id=0, has_side_effects=True, vmem_limit_bytes=40 * 1024 * 1024
        ),
    )(*[pltpu.with_memory_space_constraint(a, pltpu.HBM) for a in operands])
    anywhere = pl.BlockSpec(memory_space=pl.ANY)
    out_x, out_b, out_c, out_w = pl.pallas_call(
        ship,
        out_shape=[jax.ShapeDtypeStruct(r.shape, r.dtype) for r in results],
        in_specs=[anywhere] * 4,
        out_specs=[anywhere] * 4,
        scratch_shapes=[dma((4,))],
        compiler_params=pltpu.CompilerParams(vmem_limit_bytes=1024 * 1024),
    )(*results)
    return (out_x[None], out_b[None], out_c[None], out_w.T)


def solution(mesh):
    blocks = P("fsdp", "seq", None)
    rows = P("fsdp", None)

    def local(*args):
        nf = lax.axis_size("fsdp")
        shard = args[1].shape[0]
        lanes = args[4].shape[2] * STATE // args[5].shape[2]
        several = args[5].shape[2] // STATE > 2
        fits = several and shard % 128 == 0 and nf & (nf - 1) == 0 and lanes % (2 * QUARTER) == 0
        return (body if fits else general_body)(*args)

    return jax.shard_map(
        local,
        mesh=mesh,
        in_specs=(blocks, rows, P(), P(), blocks, blocks, blocks, blocks),
        out_specs=(blocks, blocks, blocks, rows),
        check_vma=False,
    )
```

```python
import functools

import jax
import jax.numpy as jnp
from jax import lax
from jax.experimental import pallas as pl
from jax.experimental.pallas import tpu as pltpu
from jax.sharding import PartitionSpec as P

STATE = 128
F32 = jnp.float32
BF16 = jnp.bfloat16
MESH = pl.DeviceIdType.MESH
HIGH = lax.Precision.HIGHEST


def dot(a, b, ca=1, cb=0, precision=None):
    return lax.dot_general(
        a, b, (((ca,), (cb,)), ((), ())), precision=precision, preferred_element_type=F32
    )


def halves(value, axis):
    high = value.astype(BF16)
    low = (value - high.astype(F32)).astype(BF16)
    return jnp.concatenate([high, low], axis=axis)


def iota(shape, dim):
    return lax.broadcasted_iota(jnp.int32, shape, dim)


QUARTER = 128
PIECE = 128
AHEAD = 1
LOG2_E = 1.4426950408889634


def kernel(
    nf,
    ns,
    tokens_hbm,
    weight_hbm,
    bias_hbm,
    rate_hbm,
    x_hbm,
    b_hbm,
    c_hbm,
    dy_hbm,
    out_x,
    out_b,
    out_c,
    out_w,
    tokens,
    bias,
    rate_row,
    x,
    b_in,
    c_out,
    dy,
    in_sem,
    own_sem,
    gathered,
    gathered_x,
    gathered_r,
    bias_t,
    rate_t,
    raw_t,
    cum_t,
    step_t,
    block_t,
    cum_g,
    step_g,
    decay_g,
    meet_g,
    spread_s,
    spread_st,
    state_loc,
    grad_loc,
    xs_g,
    ds_g,
    entry,
    later,
    send_f,
    send_b,
    through,
    joint,
    grad_b,
    grad_c,
    col_t,
    xt_t,
    xc_t,
    ent_t,
    z_recv,
    ag_ssem,
    ag_rsem,
    x_ssem,
    x_rsem,
    r_ssem,
    r_rsem,
    f_ssem,
    f_rsem,
    b_ssem,
    b_rsem,
    z_ssem,
    z_rsem,
):
    f = lax.axis_index("fsdp")
    z = lax.axis_index("seq")
    length = tokens.shape[0]
    heads, rows = weight_hbm.shape
    groups = b_in.shape[1] // STATE
    per = heads // groups
    wide = x.shape[1] // groups
    size = wide // per
    quarters = wide // QUARTER
    parts = wide // PIECE
    few = QUARTER // size
    bits = nf.bit_length() - 1
    last = groups - 1

    def partner(m):
        return f + sum(
            (1 - 2 * ((f // 2**j) % 2)) * 2**j for j in range(bits) if (m // 2**j) % 2
        )

    near_first = sorted(range(1, nf), key=lambda m: bin(m // 2).count("1"))
    far_first = near_first[::-1]

    own_weight = pltpu.make_async_copy(weight_hbm, gathered.at[f], own_sem.at[0])
    own_weight.start()
    barrier = pltpu.get_barrier_semaphore()
    for m in far_first:
        pl.semaphore_signal(
            barrier, inc=1, device_id={"fsdp": partner(m)}, device_id_type=MESH
        )

    @pl.when(z < ns - 1)
    def _():
        pl.semaphore_signal(
            barrier, inc=1, device_id={"seq": z + 1}, device_id_type=MESH
        )

    @pl.when(z > 0)
    def _():
        pl.semaphore_signal(
            barrier, inc=1, device_id={"seq": z - 1}, device_id_type=MESH
        )

    loads = [
        pltpu.make_async_copy(source, target, in_sem.at[n])
        for n, (source, target) in enumerate(
            (
                (bias_hbm, bias),
                (rate_hbm, rate_row),
                (tokens_hbm, tokens),
                (x_hbm, x),
                (b_hbm, b_in),
                (dy_hbm, dy),
                (c_hbm, c_out),
            )
        )
    ]
    for load in loads:
        load.start()
    loads[0].wait()
    loads[1].wait()
    bias_t[...] = jnp.broadcast_to(bias[...], (length, heads)).T
    rate_t[...] = jnp.broadcast_to(rate_row[...], (length, heads)).T
    own_weight.wait()
    ends = (z > 0).astype(jnp.int32) + (z < ns - 1).astype(jnp.int32)
    pl.semaphore_wait(barrier, nf - 1 + ends)

    def span_of(g, width):
        start = g * width
        return pl.ds(start if isinstance(start, int) else pl.multiple_of(start, width), width)

    def weight_copy(g, m):
        part = gathered.at[f, span_of(g, per)]
        return pltpu.make_async_remote_copy(
            src_ref=part,
            dst_ref=part,
            send_sem=ag_ssem.at[g, m - 1],
            recv_sem=ag_rsem.at[g, m - 1],
            device_id={"fsdp": partner(m)},
            device_id_type=MESH,
        )

    def token_copy(m):
        return pltpu.make_async_remote_copy(
            src_ref=tokens.at[:, span_of(partner(m), rows)],
            dst_ref=gathered_x.at[span_of(f, length)],
            send_sem=x_ssem.at[m - 1],
            recv_sem=x_rsem.at[m - 1],
            device_id={"fsdp": partner(m)},
            device_id_type=MESH,
        )

    def raw_copy(g, m):
        part = gathered_r.at[f, span_of(g, per)]
        return pltpu.make_async_remote_copy(
            src_ref=part,
            dst_ref=part,
            send_sem=r_ssem.at[g, m - 1],
            recv_sem=r_rsem.at[g, m - 1],
            device_id={"fsdp": partner(m)},
            device_id_type=MESH,
        )

    for m in far_first:
        weight_copy(0, m).start()
    for load in loads[2:]:
        load.wait()
    own_tokens = pltpu.make_async_copy(
        tokens.at[:, span_of(f, rows)], gathered_x.at[span_of(f, length)], own_sem.at[1]
    )
    own_tokens.start()

    @pl.when(z == 0)
    def _():
        entry[...] = jnp.zeros_like(entry)

    @pl.when(z == ns - 1)
    def _():
        later[...] = jnp.zeros_like(later)

    spread_one = (iota((2 * per, wide), 0) % per == iota((2 * per, wide), 1) // size).astype(BF16)
    gather_one = (iota((per, wide), 0) == iota((per, wide), 1) // size).astype(BF16)

    def expand(value):
        return dot(halves(value, 1), spread_one)

    def head_sums(value):
        width = value.shape[1]
        ones = (iota((width // size, width), 0) == iota((width // size, width), 1) // size).astype(BF16)
        high = value.astype(BF16)
        low = (value - high.astype(F32)).astype(BF16)
        return dot(ones, high, 1, 1) + dot(ones, low, 1, 1)

    def part(p):
        return slice(p * PIECE, (p + 1) * PIECE)

    def strip(q):
        return slice(q * QUARTER, (q + 1) * QUARTER)

    def forward_copy(g, p):
        return pltpu.make_async_remote_copy(
            src_ref=send_f.at[g, part(p)],
            dst_ref=entry.at[g, part(p)],
            send_sem=f_ssem.at[g, p],
            recv_sem=f_rsem.at[g, p],
            device_id={"seq": (z + 1) % ns},
            device_id_type=MESH,
        )

    def backward_copy(g, p):
        return pltpu.make_async_remote_copy(
            src_ref=send_b.at[g, part(p)],
            dst_ref=later.at[g, part(p)],
            send_sem=b_ssem.at[g, p],
            recv_sem=b_rsem.at[g, p],
            device_id={"seq": (z + ns - 1) % ns},
            device_id_type=MESH,
        )

    def thirds(value, axis):
        high = value.astype(BF16)
        rest = value - high.astype(F32)
        middle = rest.astype(BF16)
        low = (rest - middle.astype(F32)).astype(BF16)
        return jnp.concatenate([high, middle, low], axis=axis)

    def steps(g, product):
        mine = span_of(g, per)
        raw = bias_t[mine] + product
        step = jnp.maximum(raw, 0.0) + jnp.log1p(jnp.exp(-jnp.abs(raw)))
        before = iota((3 * length, length), 0) % length <= iota((3 * length, length), 1)
        cum = dot(thirds(-LOG2_E * rate_t[mine] * step, 1), before.astype(BF16))
        both = jnp.concatenate([cum, step], axis=0).T
        cum_c = both[:, :per]
        step_c = both[:, per:]
        cum_g[g] = cum_c
        step_g[g] = step_c
        raw_t[mine] = raw
        cum_t[mine] = cum
        step_t[mine] = step
        block_t[mine] = jnp.broadcast_to(jnp.exp2(cum[:, length - 1 : length]), (per, STATE))
        return cum_c, step_c

    def gather(g):
        for m in far_first:
            weight_copy(g, m).start()

    def prepare_first():
        mine = span_of(0, per)
        product = dot(gathered[f, mine], tokens[:, span_of(f, rows)], 1, 1)
        for n, m in enumerate(near_first):
            weight_copy(0, m).wait_recv()
            if n == 0:
                gather(1)
            elif n == nf // 2:
                gather(2)
            own = partner(m)
            product = product + dot(gathered[own, mine], tokens[:, span_of(own, rows)], 1, 1)
        for g in range(3, groups):
            gather(g)
        return steps(0, product)

    def prepare(g):
        for m in near_first:
            weight_copy(g, m).wait_recv()
        mine = span_of(g, per)
        weight = jnp.concatenate([gathered[own, mine] for own in range(nf)], axis=1)
        steps(g, dot(weight, tokens[...], 1, 1))

        @pl.when(g == 2)
        def _():
            for m in near_first[: nf // 2]:
                token_copy(m).start()

        @pl.when(g == 3)
        def _():
            for m in near_first[nf // 2 :]:
                token_copy(m).start()

    def local(g, cum_c, step_c, opening=False):
        scale = expand(step_c * jnp.exp2(cum_c[length - 1 : length] - cum_c))
        b = b_in[:, span_of(g, STATE)]
        c = c_out[:, span_of(g, STATE)]
        xs = (x[:, span_of(g, wide)].astype(F32) * scale).astype(BF16)
        ds = (dy[:, span_of(g, wide)].astype(F32) * expand(jnp.exp2(cum_c))).astype(BF16)
        state = dot(xs, b, 0, 0)
        grad = dot(ds, c, 0, 0)
        spread_st[g] = scale
        xs_g[g] = xs
        ds_g[g] = ds

        @pl.when(z == 0)
        def _():
            send_f[g] = state.astype(BF16)
            if opening:
                for p in range(AHEAD):
                    forward_copy(g, p).start()

        @pl.when(z == ns - 1)
        def _():
            send_b[g] = grad.astype(BF16)
            if opening:
                for p in range(AHEAD):
                    backward_copy(g, p).start()

        state_loc[g] = state
        grad_loc[g] = grad
        decay_g[g] = dot(spread_one, halves(block_t[span_of(g, per)], 0), 0, 0)
        spread_s[g] = expand(step_c)
        meet_g[g] = dot(b, c, 1, 1)

    def chain_f(g, p):
        @pl.when(z > 0)
        def _():
            forward_copy(g, p).wait_recv()

        @pl.when(jnp.logical_and(z > 0, z < ns - 1))
        def _():
            s = part(p)
            send_f[g, s] = (decay_g[g, s] * entry[g, s].astype(F32) + state_loc[g, s]).astype(BF16)

        @pl.when(z < ns - 1 if p >= AHEAD else (z < ns - 1) & ((z > 0) | (g > 0)))
        def _():
            forward_copy(g, p).start()

    def chain_b(g, p):
        @pl.when(z < ns - 1)
        def _():
            backward_copy(g, p).wait_recv()

        @pl.when(jnp.logical_and(z > 0, z < ns - 1))
        def _():
            s = part(p)
            send_b[g, s] = (decay_g[g, s] * later[g, s].astype(F32) + grad_loc[g, s]).astype(BF16)

        @pl.when(z > 0 if p >= AHEAD else (z > 0) & ((z < ns - 1) | (g > 0)))
        def _():
            backward_copy(g, p).start()

    def columns(g, q):
        return pl.ds(pl.multiple_of(g * wide + q * QUARTER, QUARTER), QUARTER)

    def heavy(g, q0, n):
        meet = meet_g[g]
        upper = iota((length, length), 0) <= iota((length, length), 1)
        lanes = iota((length, QUARTER), 1)
        cum_r = cum_t[span_of(g, per)]
        cum_l = cum_g[g]
        step_l = step_g[g]
        total = jnp.zeros((length, length), F32) if q0 == 0 else joint[...]
        for q in range(q0, q0 + n):
            x_q = x[:, columns(g, q)]
            dy_q = dy[:, columns(g, q)]
            sums = []
            weights = []
            masked = []
            split = [jnp.where(lanes // size == j, x_q, jnp.zeros_like(x_q)) for j in range(few)]
            pairs = dot(jnp.concatenate(split, axis=0), dy_q, 1, 1)
            for j in range(few):
                k = q * few + j
                mine = lanes // size == j
                pair = pairs[j * length : (j + 1) * length]
                spread = cum_r[k : k + 1] - cum_l[:, k : k + 1]
                decay = jnp.exp2(jnp.where(upper, spread, -1e30))
                weights.append((decay * meet).astype(BF16))
                masked.append(jnp.where(mine, dy_q, jnp.zeros_like(dy_q)))
                scaled = decay * pair * step_l[:, k : k + 1]
                total = total + scaled
                sums.append(jnp.sum(scaled * meet, axis=0, keepdims=True))
            passed = dot(jnp.concatenate(weights, axis=1), jnp.concatenate(masked, axis=0))
            through[g, :, strip(q)] = spread_s[g, :, strip(q)] * passed
            col_t[g, q] = jnp.concatenate(sums, axis=0)
            xt_t[g, q] = head_sums(x_q.astype(F32) * passed)
        if q0 + n < quarters:
            joint[...] = total
        else:
            total = total.astype(BF16)
            grad_b[g] = dot(total, c_out[:, span_of(g, STATE)])
            grad_c[g] = dot(total, b_in[:, span_of(g, STATE)], 0, 0)

    def store_sums(target, g, q, sums):
        for i in range(sums.shape[0] // few):
            target[g, q + i] = sums[i * few : (i + 1) * few]

    def sums_f(g, q):
        read = dot(c_out[:, span_of(g, STATE)], entry[g, strip(q)], 1, 1)
        store_sums(ent_t, g, q, head_sums(ds_g[g, :, strip(q)].astype(F32) * read))

    def sums_b(g, q):
        carried = dot(b_in[:, span_of(g, STATE)], later[g, strip(q)], 1, 1)
        store_sums(xc_t, g, q, head_sums(x[:, columns(g, q)].astype(F32) * carried))

    def results_f(g):
        out_c[:, span_of(g, STATE)] = (grad_c[g] + dot(ds_g[g], entry[g])).astype(BF16)

    def results_b(g):
        channels = span_of(g, wide)
        carried = dot(b_in[:, span_of(g, STATE)], later[g], 1, 1)
        out_x[:, channels] = (through[g] + spread_st[g] * carried).astype(BF16)
        out_b[:, span_of(g, STATE)] = (grad_b[g] + dot(xs_g[g], later[g])).astype(BF16)

    def finish_f(g):
        columns = span_of(g, STATE)

        @pl.when(z == 0)
        def _():
            ent_t[g] = jnp.zeros((quarters, few, length), F32)
            out_c[:, columns] = grad_c[g].astype(BF16)

        @pl.when(z > 0)
        def _():
            state = entry[g]
            ds = ds_g[g]
            read = dot(c_out[:, columns], state, 1, 1)
            store_sums(ent_t, g, 0, head_sums(ds.astype(F32) * read))
            out_c[:, columns] = (grad_c[g] + dot(ds, state)).astype(BF16)

    def finish_b(g):
        columns = span_of(g, STATE)
        channels = span_of(g, wide)

        @pl.when(z == ns - 1)
        def _():
            xc_t[g] = jnp.zeros((quarters, few, length), F32)
            out_x[:, channels] = through[g].astype(BF16)
            out_b[:, columns] = grad_b[g].astype(BF16)

        @pl.when(z < ns - 1)
        def _():
            grad = later[g]
            carried = dot(b_in[:, columns], grad, 1, 1)
            store_sums(xc_t, g, 0, head_sums(x[:, channels].astype(F32) * carried))
            out_x[:, channels] = (through[g] + spread_st[g] * carried).astype(BF16)
            out_b[:, columns] = (grad_b[g] + dot(xs_g[g], grad)).astype(BF16)

    def post(g):
        mine = span_of(g, per)
        crossing = dot(
            gather_one, (entry[g].astype(F32) * later[g].astype(F32)).astype(BF16)
        )
        cum = cum_t[mine]
        step = step_t[mine]
        rate = rate_t[mine]

        def stacked(parts):
            return jnp.concatenate([parts[g, q] for q in range(quarters)], axis=0)

        xt = stacked(xt_t)
        tail_xc = jnp.exp2(cum[:, length - 1 : length] - cum) * stacked(xc_t)
        leaving = step * tail_xc
        grad_cum = stacked(col_t) - step * xt + stacked(ent_t) - leaving
        closing = block_t[mine, :1] * jnp.sum(crossing, axis=1, keepdims=True) + jnp.sum(
            leaving, axis=1, keepdims=True
        )
        after = iota((3 * length, length), 0) % length >= iota((3 * length, length), 1)
        grad_log = dot(thirds(grad_cum, 1), after.astype(BF16)) + closing
        grad_raw = (xt + tail_xc - rate * grad_log) * jax.nn.sigmoid(raw_t[mine])
        gathered_r[f, mine] = grad_raw.astype(BF16)
        for m in far_first:
            raw_copy(g, m).start()

    def within(g):
        return jnp.logical_and(g >= 0, g < groups)

    furthest = jnp.maximum(z, ns - 1 - z)

    def slot_step(tau, carry):
        gf = tau - z
        gb = tau - (ns - 1 - z)
        whole = tau - furthest
        half = quarters // 2
        early = tau + 1 < groups
        edge = furthest == ns - 1
        lag = tau <= groups + 1
        now = (tau > groups) & ~edge
        at_front = (z == 0) & (tau > groups) & within(gb)
        at_back = (z == ns - 1) & (tau > groups) & within(gf)
        first = jnp.where(edge | (tau < 2), tau, jnp.where(tau == 2, -1, tau - 1))
        second = jnp.where(edge | (tau < 1), tau, jnp.where(tau == 1, -1, tau - 1))
        done_f = gf - 1
        done_b = gb - 1
        done = whole - 1
        stride = parts // 4
        for p in range(parts):
            pl.when(within(gf))(lambda: chain_f(gf, p))
            pl.when(within(gb))(lambda: chain_b(gb, p))
            if (p + 1) % (parts // quarters) == 0 and p + 1 < parts:
                q = p * quarters // parts
                pl.when(at_front)(lambda: sums_b(gb, q))
                pl.when(at_back)(lambda: sums_f(gf, q))
            if p == stride - 1:
                pl.when(early)(lambda: prepare(tau + 1))
                pl.when(within(done_f) & lag & ~early)(lambda: finish_f(done_f))
            elif p == 2 * stride - 1:
                pl.when(within(first))(lambda: heavy(first, 0, half))
                pl.when(within(done_f) & early)(lambda: finish_f(done_f))
            elif p == 3 * stride - 1:
                pl.when(early)(lambda: local(tau + 1, cum_g[tau + 1], step_g[tau + 1]))
                pl.when(within(done_b) & lag)(lambda: finish_b(done_b))
                pl.when(within(done) & lag)(lambda: post(done))
            elif p == 4 * stride - 1:
                pl.when(within(second))(lambda: heavy(second, half, quarters - half))

        @pl.when(at_front)
        def _():
            sums_b(gb, quarters - 1)
            post(gb)
            results_b(gb)

        @pl.when(at_back)
        def _():
            sums_f(gf, quarters - 1)
            post(gf)
            results_f(gf)

        pl.when(now & within(gf))(lambda: finish_f(gf))
        pl.when(now & within(gb))(lambda: finish_b(gb))
        pl.when(now & within(whole))(lambda: post(whole))
        return carry

    local(0, *prepare_first(), opening=True)
    lax.fori_loop(0, groups + ns - 1, slot_step, 0)

    def product(first, count):
        raws = jnp.concatenate(
            [gathered_r[own, first * per : (first + count) * per] for own in range(nf)], axis=1
        )
        return dot(raws, gathered_x[...])

    def product_as_they_come(g):
        def term(own):
            return dot(gathered_r[own, span_of(g, per)], gathered_x[span_of(own, length)])

        total = term(f)
        for m in near_first:
            raw_copy(g, m).wait_recv()
            total = total + term(partner(m))
        return total

    own_tokens.wait()
    for m in range(1, nf):
        token_copy(m).wait_recv()
    shares = []
    for n, (first, count) in enumerate(((0, groups - 2), (groups - 2, 1), (groups - 1, 1))):
        place = slice(first * per, (first + count) * per)
        if first == last:
            z_recv[z, place] = product_as_they_come(last).astype(BF16)
        else:
            for g in range(first, first + count):
                for m in range(1, nf):
                    raw_copy(g, m).wait_recv()
            z_recv[z, place] = product(first, count).astype(BF16)
        copies = []
        for d in range(1, ns):
            share = z_recv.at[z, place]
            copy = pltpu.make_async_remote_copy(
                src_ref=share,
                dst_ref=share,
                send_sem=z_ssem.at[n, d - 1],
                recv_sem=z_rsem.at[n, d - 1],
                device_id={"seq": (z + d) % ns},
                device_id_type=MESH,
            )
            copy.start()
            copies.append(copy)
        shares.append((place, copies))
    for m in range(1, nf):
        token_copy(m).wait_send()
        for g in range(groups):
            weight_copy(g, m).wait_send()
            raw_copy(g, m).wait_send()

    @pl.when(z < ns - 1)
    def _():
        for g in range(groups):
            for p in range(parts):
                forward_copy(g, p).wait_send()

    @pl.when(z > 0)
    def _():
        for g in range(groups):
            for p in range(parts):
                backward_copy(g, p).wait_send()

    for place, copies in shares:
        for copy in copies:
            copy.wait_recv()
        summed = z_recv[0, place].astype(F32)
        for k in range(1, ns):
            summed = summed + z_recv[k, place].astype(F32)
        out_w[place] = summed

    for _, copies in shares:
        for copy in copies:
            copy.wait_send()


def ship(*refs):
    sems = refs[-1]
    count = len(refs) // 2
    copies = [
        pltpu.make_async_copy(refs[n], refs[count + n], sems.at[n]) for n in range(count)
    ]
    for copy in copies:
        copy.start()
    for copy in copies:
        copy.wait()


def general_kernel(
    nf,
    ns,
    tokens_hbm,
    weight_t,
    bias,
    rate_row,
    x_hbm,
    b_hbm,
    c_hbm,
    dy_hbm,
    x_out,
    b_out,
    c_out_hbm,
    out_w,
    tokens,
    x,
    b_in,
    c_out,
    dy,
    out_x,
    out_b,
    out_c,
    in_sem,
    out_sem,
    gathered,
    raw_t,
    cum_t,
    step_t,
    block_t,
    cum_g,
    step_g,
    tail_g,
    lead_g,
    state_loc,
    grad_loc,
    xs_g,
    ds_g,
    entry,
    later,
    send_f,
    send_b,
    through,
    grad_b,
    grad_c,
    col_t,
    xt_t,
    xc_t,
    ent_t,
    total,
    rs_send,
    rs_recv,
    z_recv,
    ag_ssem,
    ag_rsem,
    f_ssem,
    f_rsem,
    b_ssem,
    b_rsem,
    rs_ssem,
    rs_rsem,
    z_ssem,
    z_rsem,
):
    f = lax.axis_index("fsdp")
    z = lax.axis_index("seq")
    length = tokens.shape[0]
    heads, rows = weight_t.shape
    groups = b_in.shape[1] // STATE
    per = heads // groups
    wide = x.shape[1] // groups
    size = wide // per
    bits = nf.bit_length() - 1
    part_heads = heads // 2
    chunk = wide // 2
    loads = [
        pltpu.make_async_copy(source, target, in_sem.at[n])
        for n, (source, target) in enumerate(
            (
                (tokens_hbm, tokens),
                (x_hbm, x),
                (dy_hbm, dy),
                (b_hbm, b_in),
                (c_hbm, c_out),
            )
        )
    ]
    for load in loads:
        load.start()
    orders = (list(reversed(range(bits))), list(range(1, bits)) + [0])

    def slot_of(index, order):
        return sum(((index // 2**b) % 2) * 2**i for i, b in enumerate(order))

    def partner(j):
        return f + (1 - 2 * ((f // 2**j) % 2)) * 2**j

    barrier = pltpu.get_barrier_semaphore()
    for j in range(bits):
        pl.semaphore_signal(
            barrier, inc=1, device_id={"fsdp": partner(j)}, device_id_type=MESH
        )
    for d in range(1, ns):
        pl.semaphore_signal(
            barrier, inc=1, device_id={"seq": (z + d) % ns}, device_id_type=MESH
        )
    pl.semaphore_wait(barrier, bits + ns - 1)

    slots = [slot_of(f, order) for order in orders]
    for h in range(2):
        gathered[h, slots[h]] = weight_t[h * part_heads : (h + 1) * part_heads]
    for i in range(bits):
        copies = []
        for h in range(2):
            part = gathered.at[h, pl.ds((slots[h] // 2**i) * 2**i, 2**i)]
            copy = pltpu.make_async_remote_copy(
                src_ref=part,
                dst_ref=part,
                send_sem=ag_ssem.at[h, i],
                recv_sem=ag_rsem.at[h, i],
                device_id={"fsdp": partner(orders[h][i])},
                device_id_type=MESH,
            )
            copy.start()
            copies.append(copy)
        if i == bits - 1:
            for load in loads:
                load.wait()
        for copy in copies:
            copy.wait()

    raw = jnp.broadcast_to(bias[...], (length, heads)).T
    rate = jnp.broadcast_to(rate_row[...], (length, heads)).T
    for own in range(nf):
        weight = jnp.concatenate(
            [gathered[h, slot_of(own, orders[h])] for h in range(2)], axis=0
        )
        raw = raw + dot(weight, tokens[:, own * rows : (own + 1) * rows], 1, 1)
    step = jnp.maximum(raw, 0.0) + jnp.log1p(jnp.exp(-jnp.abs(raw)))
    before = iota((length, length), 0) <= iota((length, length), 1)
    cum = dot(-rate * step, before.astype(F32), precision=HIGH)
    raw_t[...] = raw
    cum_t[...] = cum
    step_t[...] = step
    final = cum[:, length - 1 : length]
    block_t[...] = jnp.broadcast_to(jnp.exp(final), (heads, STATE))
    both = jnp.concatenate([cum, step], axis=0).T
    cum_c = both[:, :heads]
    step_c = both[:, heads:]
    tail_c = jnp.exp(cum_c[length - 1 : length] - cum_c)
    lead_c = jnp.exp(cum_c)
    for g in range(groups):
        span = slice(g * per, (g + 1) * per)
        cum_g[g] = cum_c[:, span]
        step_g[g] = step_c[:, span]
        tail_g[g] = tail_c[:, span]
        lead_g[g] = lead_c[:, span]

    spread_one = (iota((2 * per, wide), 0) % per == iota((2 * per, wide), 1) // size).astype(BF16)
    gather_one = (iota((per, wide), 0) == iota((per, wide), 1) // size).astype(BF16)

    def expand(value):
        return dot(halves(value, 1), spread_one)

    def head_sums(value):
        high = value.astype(BF16)
        low = (value - high.astype(F32)).astype(BF16)
        return dot(gather_one, high, 1, 1) + dot(gather_one, low, 1, 1)

    def span_of(g, width):
        return pl.ds(pl.multiple_of(g * width, width), width)

    @pl.when(z == 0)
    def _():
        entry[...] = jnp.zeros_like(entry)

    @pl.when(z == ns - 1)
    def _():
        later[...] = jnp.zeros_like(later)

    spread_half = (
        iota((per, chunk), 0) % (per // 2) == iota((per, chunk), 1) // size
    ).astype(BF16)

    def piece(g):
        return g // 2, pl.ds(pl.multiple_of((g % 2) * chunk, chunk), chunk)

    def forward_copy(g):
        return pltpu.make_async_remote_copy(
            src_ref=send_f.at[piece(g)],
            dst_ref=entry.at[piece(g)],
            send_sem=f_ssem.at[g],
            recv_sem=f_rsem.at[g],
            device_id={"seq": (z + 1) % ns},
            device_id_type=MESH,
        )

    def backward_copy(g):
        return pltpu.make_async_remote_copy(
            src_ref=send_b.at[piece(g)],
            dst_ref=later.at[piece(g)],
            send_sem=b_ssem.at[g],
            recv_sem=b_rsem.at[g],
            device_id={"seq": (z + ns - 1) % ns},
            device_id_type=MESH,
        )

    def local(g):
        xs = (x[:, span_of(g, wide)].astype(F32) * expand(step_g[g] * tail_g[g])).astype(BF16)
        ds = (dy[:, span_of(g, wide)].astype(F32) * expand(lead_g[g])).astype(BF16)
        xs_g[g] = xs
        ds_g[g] = ds
        state_loc[g] = dot(xs, b_in[:, span_of(g, STATE)], 0, 0)
        grad_loc[g] = dot(ds, c_out[:, span_of(g, STATE)], 0, 0)

    def decay_rows(g):
        return dot(spread_half, halves(block_t[span_of(g, per // 2)], 0), 0, 0)

    def chain_f(g):
        @pl.when(z > 0)
        def _():
            forward_copy(g).wait_recv()

        @pl.when(z < ns - 1)
        def _():
            p = piece(g)
            send_f[p] = (decay_rows(g) * entry[p].astype(F32) + state_loc[p]).astype(BF16)
            forward_copy(g).start()

    def chain_b(g):
        @pl.when(z < ns - 1)
        def _():
            backward_copy(g).wait_recv()

        @pl.when(z > 0)
        def _():
            p = piece(g)
            send_b[p] = (decay_rows(g) * later[p].astype(F32) + grad_loc[p]).astype(BF16)
            backward_copy(g).start()

    def heavy(g):
        inputs = x[:, span_of(g, wide)]
        upstream = dy[:, span_of(g, wide)]
        b = b_in[:, span_of(g, STATE)]
        c = c_out[:, span_of(g, STATE)]
        meet = dot(b, c, 1, 1)
        upper = iota((length, length), 0) <= iota((length, length), 1)
        lanes = iota((length, 128), 1)
        cum_r = cum_t[span_of(g, per)]
        cum_l = cum_g[g]
        step_l = step_g[g]
        joint = jnp.zeros((length, length), F32)
        sums = []
        pieces = []
        for q in range(wide // 128):
            x_q = inputs[:, q * 128 : (q + 1) * 128]
            dy_q = upstream[:, q * 128 : (q + 1) * 128]
            weights = []
            masked = []
            for j in range(128 // size):
                k = q * (128 // size) + j
                mine = lanes // size == j
                pair = dot(jnp.where(mine, x_q, jnp.zeros_like(x_q)), dy_q, 1, 1)
                spread = cum_r[k : k + 1] - cum_l[:, k : k + 1]
                decay = jnp.exp(jnp.where(upper, spread, -1e30))
                weights.append((decay * meet).astype(BF16))
                masked.append(jnp.where(mine, dy_q, jnp.zeros_like(dy_q)))
                scaled = decay * pair * step_l[:, k : k + 1]
                joint = joint + scaled
                sums.append(jnp.sum(scaled * meet, axis=0, keepdims=True))
            pieces.append(
                dot(jnp.concatenate(weights, axis=1), jnp.concatenate(masked, axis=0))
            )
        passed = jnp.concatenate(pieces, axis=1)
        through[g] = passed
        col_t[span_of(g, per)] = jnp.concatenate(sums, axis=0)
        xt_t[span_of(g, per)] = head_sums(inputs.astype(F32) * passed)
        joint = joint.astype(BF16)
        grad_b[g] = dot(joint, c)
        grad_c[g] = dot(joint, b, 0, 0)

    def finish_f(g):
        c = c_out[:, span_of(g, STATE)]
        read = dot(c, entry[g], 1, 1)
        ent_t[span_of(g, per)] = head_sums(ds_g[g].astype(F32) * read)
        out_c[:, span_of(g, STATE)] = (grad_c[g] + dot(ds_g[g], entry[g])).astype(BF16)

    def finish_b(g):
        b = b_in[:, span_of(g, STATE)]
        carried = dot(b, later[g], 1, 1)
        xc_t[span_of(g, per)] = head_sums(x[:, span_of(g, wide)].astype(F32) * carried)
        inner = through[g] + expand(tail_g[g]) * carried
        out_x[:, span_of(g, wide)] = (expand(step_g[g]) * inner).astype(BF16)
        out_b[:, span_of(g, STATE)] = (grad_b[g] + dot(xs_g[g], later[g])).astype(BF16)

    def within(g):
        return jnp.logical_and(g >= 0, g < groups)

    def slot_step(tau, carry):
        gf = tau - z
        gb = tau - (ns - 1 - z)
        pl.when(tau < groups)(lambda: local(tau))
        pl.when(within(gf))(lambda: chain_f(2 * gf))
        pl.when(within(gb))(lambda: chain_b(2 * gb))
        pl.when(tau < groups)(lambda: heavy(tau))
        pl.when(within(gf))(lambda: chain_f(2 * gf + 1))
        pl.when(within(gb))(lambda: chain_b(2 * gb + 1))
        pl.when(within(gf))(lambda: finish_f(gf))
        pl.when(within(gb))(lambda: finish_b(gb))
        return carry

    lax.fori_loop(0, groups + ns - 1, slot_step, 0)
    stores = [
        pltpu.make_async_copy(source, target, out_sem.at[n])
        for n, (source, target) in enumerate(
            ((out_x, x_out), (out_b, b_out), (out_c, c_out_hbm))
        )
    ]
    for store in stores:
        store.start()

    crossing = jnp.concatenate(
        [
            dot(gather_one, (entry[g].astype(F32) * later[g].astype(F32)).astype(BF16))
            for g in range(groups)
        ],
        axis=0,
    )
    cum = cum_t[...]
    step = step_t[...]
    raw = raw_t[...]
    tail = jnp.exp(cum[:, length - 1 : length] - cum)
    xt = xt_t[...]
    tail_xc = tail * xc_t[...]
    leaving = step * tail_xc
    grad_cum = col_t[...] - step * xt + ent_t[...] - leaving
    closing = block_t[:, :1] * jnp.sum(crossing, axis=1, keepdims=True) + jnp.sum(
        leaving, axis=1, keepdims=True
    )
    after = (iota((length, length), 0) >= iota((length, length), 1)).astype(F32)
    grad_log = dot(grad_cum, after, precision=HIGH) + closing
    grad_raw = (xt + tail_xc - rate * grad_log) * jax.nn.sigmoid(raw)
    grad_raw = grad_raw.astype(BF16)

    bases = [0, 0]
    count = nf
    early = rows % 128 == 0

    def product(own, target, place, offset):
        columns = pl.ds(pl.multiple_of(own * rows, 128), rows) if early else slice(
            own * rows, (own + 1) * rows
        )
        block = dot(grad_raw, tokens[:, columns])
        for h in range(2):
            target[h, offset + place[h]] = block[
                h * part_heads : (h + 1) * part_heads
            ].astype(target.dtype)

    for j in range(bits):
        half = count // 2
        sent = pl.ds(nf - count, half)
        if j == 0 and early:
            bit = f % 2
            for i in range(half):
                place = [slot_of(2 * i, order) for order in orders]
                product(2 * i + (1 - bit), rs_send, place, 0)
        elif j == 0:
            for own in range(nf):
                product(own, total, [slot_of(own, order) for order in orders], 0)
        copies = []
        for h in range(2):
            b = orders[h][bits - 1 - j]
            bit_h = (f // 2**b) % 2
            if j > 0 or not early:
                rs_send[h, sent] = total[
                    h, pl.ds(bases[h] + (1 - bit_h) * half, half)
                ].astype(BF16)
            copy = pltpu.make_async_remote_copy(
                src_ref=rs_send.at[h, sent],
                dst_ref=rs_recv.at[h, sent],
                send_sem=rs_ssem.at[h, j],
                recv_sem=rs_rsem.at[h, j],
                device_id={"fsdp": partner(b)},
                device_id_type=MESH,
            )
            copy.start()
            copies.append(copy)
            bases[h] = bases[h] + bit_h * half
        if j == 0 and early:
            for i in range(half):
                place = [slot_of(2 * i, order) for order in orders]
                product(2 * i + bit, total, place, bit * half)
        for h in range(2):
            copies[h].wait()
            total[h, pl.ds(bases[h], half)] += rs_recv[h, sent].astype(F32)
        count = half

    z_recv[z] = jnp.concatenate([total[h, bases[h]] for h in range(2)], axis=0).astype(BF16)
    copies = []
    for d in range(1, ns):
        copy = pltpu.make_async_remote_copy(
            src_ref=z_recv.at[z],
            dst_ref=z_recv.at[z],
            send_sem=z_ssem.at[d - 1],
            recv_sem=z_rsem.at[d - 1],
            device_id={"seq": (z + d) % ns},
            device_id_type=MESH,
        )
        copy.start()
        copies.append(copy)
    for copy in copies:
        copy.wait()
    summed = z_recv[0].astype(F32)
    for k in range(1, ns):
        summed = summed + z_recv[k].astype(F32)
    out_w[...] = summed

    @pl.when(z < ns - 1)
    def _():
        for g in range(2 * groups):
            forward_copy(g).wait_send()

    @pl.when(z > 0)
    def _():
        for g in range(2 * groups):
            backward_copy(g).wait_send()

    for store in stores:
        store.wait()


def general_body(
    layer_input, dt_weight, dt_bias, decay_rate, ssm_input, in_basis, out_basis, out_cotangent
):
    nf, ns = lax.axis_size("fsdp"), lax.axis_size("seq")
    length = layer_input.shape[1]
    rows, heads = dt_weight.shape
    groups = in_basis.shape[2] // STATE
    per = heads // groups
    full = ssm_input.shape[2]
    wide = full // groups
    bits = nf.bit_length() - 1
    tall = (groups, wide, STATE)
    dma = pltpu.SemaphoreType.DMA
    v = pltpu.VMEM
    scratch = [
        v((length, layer_input.shape[2]), BF16),
        v((length, full), BF16),
        v((length, groups * STATE), BF16),
        v((length, groups * STATE), BF16),
        v((length, full), BF16),
        v((length, full), BF16),
        v((length, groups * STATE), BF16),
        v((length, groups * STATE), BF16),
        dma((5,)),
        dma((3,)),
        v((2, nf, heads // 2, rows), BF16),
        v((heads, length), F32),
        v((heads, length), F32),
        v((heads, length), F32),
        v((heads, STATE), F32),
        v((groups, length, per), F32),
        v((groups, length, per), F32),
        v((groups, length, per), F32),
        v((groups, length, per), F32),
        v(tall, F32),
        v(tall, F32),
        v((groups, length, wide), BF16),
        v((groups, length, wide), BF16),
        v(tall, BF16),
        v(tall, BF16),
        v(tall, BF16),
        v(tall, BF16),
        v((groups, length, wide), F32),
        v((groups, length, STATE), F32),
        v((groups, length, STATE), F32),
        v((heads, length), F32),
        v((heads, length), F32),
        v((heads, length), F32),
        v((heads, length), F32),
        v((2, nf, heads // 2, rows), F32),
        v((2, nf, heads // 2, rows), BF16),
        v((2, nf, heads // 2, rows), BF16),
        v((ns, heads, rows), BF16),
        dma((2, bits)),
        dma((2, bits)),
        dma((2 * groups,)),
        dma((2 * groups,)),
        dma((2 * groups,)),
        dma((2 * groups,)),
        dma((2, bits)),
        dma((2, bits)),
        dma((ns - 1,)),
        dma((ns - 1,)),
    ]
    anywhere = pl.BlockSpec(memory_space=pl.ANY)
    inside = pl.BlockSpec(memory_space=pltpu.VMEM)
    out_x, out_b, out_c, out_w = pl.pallas_call(
        functools.partial(general_kernel, nf, ns),
        out_shape=(
            jax.ShapeDtypeStruct((length, full), BF16),
            jax.ShapeDtypeStruct((length, groups * STATE), BF16),
            jax.ShapeDtypeStruct((length, groups * STATE), BF16),
            jax.ShapeDtypeStruct((heads, rows), F32),
        ),
        in_specs=[anywhere] + [inside] * 3 + [anywhere] * 4,
        out_specs=[anywhere] * 3 + [inside],
        scratch_shapes=scratch,
        compiler_params=pltpu.CompilerParams(
            collective_id=0, has_side_effects=True, vmem_limit_bytes=60 * 1024 * 1024
        ),
    )(
        layer_input[0],
        dt_weight.T,
        dt_bias[None],
        decay_rate[None],
        ssm_input[0],
        in_basis[0],
        out_basis[0],
        out_cotangent[0],
    )
    return (out_x[None], out_b[None], out_c[None], out_w.T)


def body(
    layer_input, dt_weight, dt_bias, decay_rate, ssm_input, in_basis, out_basis, out_cotangent
):
    nf, ns = lax.axis_size("fsdp"), lax.axis_size("seq")
    length = layer_input.shape[1]
    rows, heads = dt_weight.shape
    groups = in_basis.shape[2] // STATE
    per = heads // groups
    full = ssm_input.shape[2]
    wide = full // groups
    size = wide // per
    quarters = wide // QUARTER
    parts = wide // PIECE
    few = QUARTER // size
    tall = (groups, wide, STATE)
    flat = (groups, length, wide)
    dma = pltpu.SemaphoreType.DMA
    v = pltpu.VMEM
    scratch = [
        v((length, layer_input.shape[2]), BF16),
        v((1, heads), F32),
        v((1, heads), F32),
        v((length, full), BF16),
        v((length, groups * STATE), BF16),
        v((length, groups * STATE), BF16),
        v((length, full), BF16),
        dma((7,)),
        dma((2,)),
        v((nf, heads, rows), BF16),
        v((nf * length, rows), BF16),
        v((nf, heads, length), BF16),
        v((heads, length), F32),
        v((heads, length), F32),
        v((heads, length), F32),
        v((heads, length), F32),
        v((heads, length), F32),
        v((heads, STATE), F32),
        v((groups, length, per), F32),
        v((groups, length, per), F32),
        v(tall, F32),
        v((groups, length, length), F32),
        v(flat, F32),
        v(flat, F32),
        v(tall, F32),
        v(tall, F32),
        v(flat, BF16),
        v(flat, BF16),
        v(tall, BF16),
        v(tall, BF16),
        v(tall, BF16),
        v(tall, BF16),
        v(flat, F32),
        v((length, length), F32),
        v((groups, length, STATE), F32),
        v((groups, length, STATE), F32),
        v((groups, quarters, few, length), F32),
        v((groups, quarters, few, length), F32),
        v((groups, quarters, few, length), F32),
        v((groups, quarters, few, length), F32),
        v((ns, heads, rows), BF16),
        dma((groups, nf - 1)),
        dma((groups, nf - 1)),
        dma((nf - 1,)),
        dma((nf - 1,)),
        dma((groups, nf - 1)),
        dma((groups, nf - 1)),
        dma((groups, parts)),
        dma((groups, parts)),
        dma((groups, parts)),
        dma((groups, parts)),
        dma((3, ns - 1)),
        dma((3, ns - 1)),
    ]
    inside = pl.BlockSpec(memory_space=pltpu.VMEM)
    outside = pl.BlockSpec(memory_space=pltpu.HBM)
    operands = (
        layer_input[0],
        dt_weight.T,
        dt_bias[None],
        decay_rate[None],
        ssm_input[0],
        in_basis[0],
        out_basis[0],
        out_cotangent[0],
    )
    results = pl.pallas_call(
        functools.partial(kernel, nf, ns),
        out_shape=(
            jax.ShapeDtypeStruct((length, full), BF16),
            jax.ShapeDtypeStruct((length, groups * STATE), BF16),
            jax.ShapeDtypeStruct((length, groups * STATE), BF16),
            jax.ShapeDtypeStruct((heads, rows), F32),
        ),
        in_specs=[outside] * len(operands),
        out_specs=[inside] * 4,
        scratch_shapes=scratch,
        compiler_params=pltpu.CompilerParams(
            collective_id=0, has_side_effects=True, vmem_limit_bytes=40 * 1024 * 1024
        ),
    )(*[pltpu.with_memory_space_constraint(a, pltpu.HBM) for a in operands])
    anywhere = pl.BlockSpec(memory_space=pl.ANY)
    out_x, out_b, out_c, out_w = pl.pallas_call(
        ship,
        out_shape=[jax.ShapeDtypeStruct(r.shape, r.dtype) for r in results],
        in_specs=[anywhere] * 4,
        out_specs=[anywhere] * 4,
        scratch_shapes=[dma((4,))],
        compiler_params=pltpu.CompilerParams(vmem_limit_bytes=1024 * 1024),
    )(*results)
    return (out_x[None], out_b[None], out_c[None], out_w.T)


def solution(mesh):
    blocks = P("fsdp", "seq", None)
    rows = P("fsdp", None)

    def local(*args):
        nf = lax.axis_size("fsdp")
        shard = args[1].shape[0]
        lanes = args[4].shape[2] * STATE // args[5].shape[2]
        several = args[5].shape[2] // STATE > 2
        fits = several and shard % 128 == 0 and nf & (nf - 1) == 0 and lanes % (2 * QUARTER) == 0
        return (body if fits else general_body)(*args)

    return jax.shard_map(
        local,
        mesh=mesh,
        in_specs=(blocks, rows, P(), P(), blocks, blocks, blocks, blocks),
        out_specs=(blocks, blocks, blocks, rows),
        check_vma=False,
    )
```

```python
import functools

import jax
import jax.numpy as jnp
from jax import lax
from jax.experimental import pallas as pl
from jax.experimental.pallas import tpu as pltpu
from jax.sharding import PartitionSpec as P

STATE = 128
F32 = jnp.float32
BF16 = jnp.bfloat16
MESH = pl.DeviceIdType.MESH
HIGH = lax.Precision.HIGHEST


def dot(a, b, ca=1, cb=0, precision=None):
    return lax.dot_general(
        a, b, (((ca,), (cb,)), ((), ())), precision=precision, preferred_element_type=F32
    )


def halves(value, axis):
    high = value.astype(BF16)
    low = (value - high.astype(F32)).astype(BF16)
    return jnp.concatenate([high, low], axis=axis)


def iota(shape, dim):
    return lax.broadcasted_iota(jnp.int32, shape, dim)


QUARTER = 128
PIECE = 128
AHEAD = 1
LOG2_E = 1.4426950408889634


def kernel(
    nf,
    ns,
    tokens_hbm,
    weight_hbm,
    bias_hbm,
    rate_hbm,
    x_hbm,
    b_hbm,
    c_hbm,
    dy_hbm,
    out_x,
    out_b,
    out_c,
    out_w,
    tokens,
    bias,
    rate_row,
    x,
    b_in,
    c_out,
    dy,
    in_sem,
    own_sem,
    gathered,
    gathered_x,
    gathered_r,
    bias_t,
    rate_t,
    raw_t,
    cum_t,
    step_t,
    block_t,
    cum_g,
    step_g,
    decay_g,
    meet_g,
    spread_s,
    spread_st,
    state_loc,
    grad_loc,
    xs_g,
    ds_g,
    entry,
    later,
    send_f,
    send_b,
    through,
    joint,
    grad_b,
    grad_c,
    col_t,
    xt_t,
    xc_t,
    ent_t,
    z_recv,
    ag_ssem,
    ag_rsem,
    x_ssem,
    x_rsem,
    r_ssem,
    r_rsem,
    f_ssem,
    f_rsem,
    b_ssem,
    b_rsem,
    z_ssem,
    z_rsem,
):
    f = lax.axis_index("fsdp")
    z = lax.axis_index("seq")
    length = tokens.shape[0]
    heads, rows = weight_hbm.shape
    groups = b_in.shape[1] // STATE
    per = heads // groups
    wide = x.shape[1] // groups
    size = wide // per
    quarters = wide // QUARTER
    parts = wide // PIECE
    few = QUARTER // size
    bits = nf.bit_length() - 1
    last = groups - 1

    def partner(m):
        return f + sum(
            (1 - 2 * ((f // 2**j) % 2)) * 2**j for j in range(bits) if (m // 2**j) % 2
        )

    near_first = sorted(range(1, nf), key=lambda m: bin(m // 2).count("1"))
    far_first = near_first[::-1]

    own_weight = pltpu.make_async_copy(weight_hbm, gathered.at[f], own_sem.at[0])
    own_weight.start()
    barrier = pltpu.get_barrier_semaphore()
    for m in far_first:
        pl.semaphore_signal(
            barrier, inc=1, device_id={"fsdp": partner(m)}, device_id_type=MESH
        )

    @pl.when(z < ns - 1)
    def _():
        pl.semaphore_signal(
            barrier, inc=1, device_id={"seq": z + 1}, device_id_type=MESH
        )

    @pl.when(z > 0)
    def _():
        pl.semaphore_signal(
            barrier, inc=1, device_id={"seq": z - 1}, device_id_type=MESH
        )

    loads = [
        pltpu.make_async_copy(source, target, in_sem.at[n])
        for n, (source, target) in enumerate(
            (
                (bias_hbm, bias),
                (rate_hbm, rate_row),
                (tokens_hbm, tokens),
                (x_hbm, x),
                (b_hbm, b_in),
                (dy_hbm, dy),
                (c_hbm, c_out),
            )
        )
    ]
    for load in loads:
        load.start()
    loads[0].wait()
    loads[1].wait()
    bias_t[...] = jnp.broadcast_to(bias[...], (length, heads)).T
    rate_t[...] = jnp.broadcast_to(rate_row[...], (length, heads)).T
    own_weight.wait()
    ends = (z > 0).astype(jnp.int32) + (z < ns - 1).astype(jnp.int32)
    pl.semaphore_wait(barrier, nf - 1 + ends)

    def span_of(g, width):
        start = g * width
        return pl.ds(start if isinstance(start, int) else pl.multiple_of(start, width), width)

    def weight_copy(g, m):
        part = gathered.at[f, span_of(g, per)]
        return pltpu.make_async_remote_copy(
            src_ref=part,
            dst_ref=part,
            send_sem=ag_ssem.at[g, m - 1],
            recv_sem=ag_rsem.at[g, m - 1],
            device_id={"fsdp": partner(m)},
            device_id_type=MESH,
        )

    def token_copy(m):
        return pltpu.make_async_remote_copy(
            src_ref=tokens.at[:, span_of(partner(m), rows)],
            dst_ref=gathered_x.at[span_of(f, length)],
            send_sem=x_ssem.at[m - 1],
            recv_sem=x_rsem.at[m - 1],
            device_id={"fsdp": partner(m)},
            device_id_type=MESH,
        )

    def raw_copy(g, m):
        part = gathered_r.at[f, span_of(g, per)]
        return pltpu.make_async_remote_copy(
            src_ref=part,
            dst_ref=part,
            send_sem=r_ssem.at[g, m - 1],
            recv_sem=r_rsem.at[g, m - 1],
            device_id={"fsdp": partner(m)},
            device_id_type=MESH,
        )

    for m in far_first:
        weight_copy(0, m).start()
    for load in loads[2:]:
        load.wait()
    own_tokens = pltpu.make_async_copy(
        tokens.at[:, span_of(f, rows)], gathered_x.at[span_of(f, length)], own_sem.at[1]
    )
    own_tokens.start()

    @pl.when(z == 0)
    def _():
        entry[...] = jnp.zeros_like(entry)

    @pl.when(z == ns - 1)
    def _():
        later[...] = jnp.zeros_like(later)

    spread_one = (iota((2 * per, wide), 0) % per == iota((2 * per, wide), 1) // size).astype(BF16)
    gather_one = (iota((per, wide), 0) == iota((per, wide), 1) // size).astype(BF16)

    def expand(value):
        return dot(halves(value, 1), spread_one)

    def head_sums(value):
        width = value.shape[1]
        ones = (iota((width // size, width), 0) == iota((width // size, width), 1) // size).astype(BF16)
        high = value.astype(BF16)
        low = (value - high.astype(F32)).astype(BF16)
        return dot(ones, high, 1, 1) + dot(ones, low, 1, 1)

    def part(p):
        return slice(p * PIECE, (p + 1) * PIECE)

    def strip(q):
        return slice(q * QUARTER, (q + 1) * QUARTER)

    def forward_copy(g, p):
        return pltpu.make_async_remote_copy(
            src_ref=send_f.at[g, part(p)],
            dst_ref=entry.at[g, part(p)],
            send_sem=f_ssem.at[g, p],
            recv_sem=f_rsem.at[g, p],
            device_id={"seq": (z + 1) % ns},
            device_id_type=MESH,
        )

    def backward_copy(g, p):
        return pltpu.make_async_remote_copy(
            src_ref=send_b.at[g, part(p)],
            dst_ref=later.at[g, part(p)],
            send_sem=b_ssem.at[g, p],
            recv_sem=b_rsem.at[g, p],
            device_id={"seq": (z + ns - 1) % ns},
            device_id_type=MESH,
        )

    def thirds(value, axis):
        high = value.astype(BF16)
        rest = value - high.astype(F32)
        middle = rest.astype(BF16)
        low = (rest - middle.astype(F32)).astype(BF16)
        return jnp.concatenate([high, middle, low], axis=axis)

    def steps(g, product):
        mine = span_of(g, per)
        raw = bias_t[mine] + product
        step = jnp.maximum(raw, 0.0) + jnp.log1p(jnp.exp(-jnp.abs(raw)))
        before = iota((3 * length, length), 0) % length <= iota((3 * length, length), 1)
        cum = dot(thirds(-LOG2_E * rate_t[mine] * step, 1), before.astype(BF16))
        both = jnp.concatenate([cum, step], axis=0).T
        cum_c = both[:, :per]
        step_c = both[:, per:]
        cum_g[g] = cum_c
        step_g[g] = step_c
        raw_t[mine] = raw
        cum_t[mine] = cum
        step_t[mine] = step
        block_t[mine] = jnp.broadcast_to(jnp.exp2(cum[:, length - 1 : length]), (per, STATE))
        return cum_c, step_c

    def gather(g):
        for m in far_first:
            weight_copy(g, m).start()

    def prepare_first():
        mine = span_of(0, per)
        product = dot(gathered[f, mine], tokens[:, span_of(f, rows)], 1, 1)
        for n, m in enumerate(near_first):
            weight_copy(0, m).wait_recv()
            if n == 0:
                gather(1)
            elif n == nf // 2:
                gather(2)
            own = partner(m)
            product = product + dot(gathered[own, mine], tokens[:, span_of(own, rows)], 1, 1)
        for g in range(3, groups):
            gather(g)
        return steps(0, product)

    def prepare(g):
        for m in near_first:
            weight_copy(g, m).wait_recv()
        mine = span_of(g, per)
        weight = jnp.concatenate([gathered[own, mine] for own in range(nf)], axis=1)
        steps(g, dot(weight, tokens[...], 1, 1))

        @pl.when(g == 2)
        def _():
            for m in near_first[: nf // 2]:
                token_copy(m).start()

        @pl.when(g == 3)
        def _():
            for m in near_first[nf // 2 :]:
                token_copy(m).start()

    def local(g, cum_c, step_c, opening=False):
        scale = expand(step_c * jnp.exp2(cum_c[length - 1 : length] - cum_c))
        b = b_in[:, span_of(g, STATE)]
        c = c_out[:, span_of(g, STATE)]
        xs = (x[:, span_of(g, wide)].astype(F32) * scale).astype(BF16)
        ds = (dy[:, span_of(g, wide)].astype(F32) * expand(jnp.exp2(cum_c))).astype(BF16)
        state = dot(xs, b, 0, 0)
        grad = dot(ds, c, 0, 0)
        spread_st[g] = scale
        xs_g[g] = xs
        ds_g[g] = ds

        @pl.when(z == 0)
        def _():
            send_f[g] = state.astype(BF16)
            if opening:
                for p in range(AHEAD):
                    forward_copy(g, p).start()

        @pl.when(z == ns - 1)
        def _():
            send_b[g] = grad.astype(BF16)
            if opening:
                for p in range(AHEAD):
                    backward_copy(g, p).start()

        state_loc[g] = state
        grad_loc[g] = grad
        decay_g[g] = dot(spread_one, halves(block_t[span_of(g, per)], 0), 0, 0)
        spread_s[g] = expand(step_c)
        meet_g[g] = dot(b, c, 1, 1)

    def chain_f(g, p):
        @pl.when(z > 0)
        def _():
            forward_copy(g, p).wait_recv()

        @pl.when(jnp.logical_and(z > 0, z < ns - 1))
        def _():
            s = part(p)
            send_f[g, s] = (decay_g[g, s] * entry[g, s].astype(F32) + state_loc[g, s]).astype(BF16)

        @pl.when(z < ns - 1 if p >= AHEAD else (z < ns - 1) & ((z > 0) | (g > 0)))
        def _():
            forward_copy(g, p).start()

    def chain_b(g, p):
        @pl.when(z < ns - 1)
        def _():
            backward_copy(g, p).wait_recv()

        @pl.when(jnp.logical_and(z > 0, z < ns - 1))
        def _():
            s = part(p)
            send_b[g, s] = (decay_g[g, s] * later[g, s].astype(F32) + grad_loc[g, s]).astype(BF16)

        @pl.when(z > 0 if p >= AHEAD else (z > 0) & ((z < ns - 1) | (g > 0)))
        def _():
            backward_copy(g, p).start()

    def columns(g, q):
        return pl.ds(pl.multiple_of(g * wide + q * QUARTER, QUARTER), QUARTER)

    def heavy(g, q0, n):
        meet = meet_g[g]
        upper = iota((length, length), 0) <= iota((length, length), 1)
        lanes = iota((length, QUARTER), 1)
        cum_r = cum_t[span_of(g, per)]
        cum_l = cum_g[g]
        step_l = step_g[g]
        total = jnp.zeros((length, length), F32) if q0 == 0 else joint[...]
        for q in range(q0, q0 + n):
            x_q = x[:, columns(g, q)]
            dy_q = dy[:, columns(g, q)]
            sums = []
            weights = []
            masked = []
            split = [jnp.where(lanes // size == j, x_q, jnp.zeros_like(x_q)) for j in range(few)]
            pairs = dot(jnp.concatenate(split, axis=0), dy_q, 1, 1)
            for j in range(few):
                k = q * few + j
                mine = lanes // size == j
                pair = pairs[j * length : (j + 1) * length]
                spread = cum_r[k : k + 1] - cum_l[:, k : k + 1]
                decay = jnp.exp2(jnp.where(upper, spread, -1e30))
                weights.append((decay * meet).astype(BF16))
                masked.append(jnp.where(mine, dy_q, jnp.zeros_like(dy_q)))
                scaled = decay * pair * step_l[:, k : k + 1]
                total = total + scaled
                sums.append(jnp.sum(scaled * meet, axis=0, keepdims=True))
            passed = dot(jnp.concatenate(weights, axis=1), jnp.concatenate(masked, axis=0))
            through[g, :, strip(q)] = spread_s[g, :, strip(q)] * passed
            col_t[g, q] = jnp.concatenate(sums, axis=0)
            xt_t[g, q] = head_sums(x_q.astype(F32) * passed)
        if q0 + n < quarters:
            joint[...] = total
        else:
            total = total.astype(BF16)
            grad_b[g] = dot(total, c_out[:, span_of(g, STATE)])
            grad_c[g] = dot(total, b_in[:, span_of(g, STATE)], 0, 0)

    def store_sums(target, g, q, sums):
        for i in range(sums.shape[0] // few):
            target[g, q + i] = sums[i * few : (i + 1) * few]

    def sums_f(g, q):
        read = dot(c_out[:, span_of(g, STATE)], entry[g, strip(q)], 1, 1)
        store_sums(ent_t, g, q, head_sums(ds_g[g, :, strip(q)].astype(F32) * read))

    def sums_b(g, q):
        carried = dot(b_in[:, span_of(g, STATE)], later[g, strip(q)], 1, 1)
        store_sums(xc_t, g, q, head_sums(x[:, columns(g, q)].astype(F32) * carried))

    def results_f(g):
        out_c[:, span_of(g, STATE)] = (grad_c[g] + dot(ds_g[g], entry[g])).astype(BF16)

    def results_b(g):
        channels = span_of(g, wide)
        carried = dot(b_in[:, span_of(g, STATE)], later[g], 1, 1)
        out_x[:, channels] = (through[g] + spread_st[g] * carried).astype(BF16)
        out_b[:, span_of(g, STATE)] = (grad_b[g] + dot(xs_g[g], later[g])).astype(BF16)

    def finish_f(g):
        columns = span_of(g, STATE)

        @pl.when(z == 0)
        def _():
            ent_t[g] = jnp.zeros((quarters, few, length), F32)
            out_c[:, columns] = grad_c[g].astype(BF16)

        @pl.when(z > 0)
        def _():
            state = entry[g]
            ds = ds_g[g]
            read = dot(c_out[:, columns], state, 1, 1)
            store_sums(ent_t, g, 0, head_sums(ds.astype(F32) * read))
            out_c[:, columns] = (grad_c[g] + dot(ds, state)).astype(BF16)

    def finish_b(g):
        columns = span_of(g, STATE)
        channels = span_of(g, wide)

        @pl.when(z == ns - 1)
        def _():
            xc_t[g] = jnp.zeros((quarters, few, length), F32)
            out_x[:, channels] = through[g].astype(BF16)
            out_b[:, columns] = grad_b[g].astype(BF16)

        @pl.when(z < ns - 1)
        def _():
            grad = later[g]
            carried = dot(b_in[:, columns], grad, 1, 1)
            store_sums(xc_t, g, 0, head_sums(x[:, channels].astype(F32) * carried))
            out_x[:, channels] = (through[g] + spread_st[g] * carried).astype(BF16)
            out_b[:, columns] = (grad_b[g] + dot(xs_g[g], grad)).astype(BF16)

    def post(g):
        mine = span_of(g, per)
        crossing = dot(
            gather_one, (entry[g].astype(F32) * later[g].astype(F32)).astype(BF16)
        )
        cum = cum_t[mine]
        step = step_t[mine]
        rate = rate_t[mine]

        def stacked(parts):
            return jnp.concatenate([parts[g, q] for q in range(quarters)], axis=0)

        xt = stacked(xt_t)
        tail_xc = jnp.exp2(cum[:, length - 1 : length] - cum) * stacked(xc_t)
        leaving = step * tail_xc
        grad_cum = stacked(col_t) - step * xt + stacked(ent_t) - leaving
        closing = block_t[mine, :1] * jnp.sum(crossing, axis=1, keepdims=True) + jnp.sum(
            leaving, axis=1, keepdims=True
        )
        after = iota((3 * length, length), 0) % length >= iota((3 * length, length), 1)
        grad_log = dot(thirds(grad_cum, 1), after.astype(BF16)) + closing
        grad_raw = (xt + tail_xc - rate * grad_log) * jax.nn.sigmoid(raw_t[mine])
        gathered_r[f, mine] = grad_raw.astype(BF16)
        for m in far_first:
            raw_copy(g, m).start()

    def within(g):
        return jnp.logical_and(g >= 0, g < groups)

    furthest = jnp.maximum(z, ns - 1 - z)

    def slot_step(tau, carry):
        gf = tau - z
        gb = tau - (ns - 1 - z)
        whole = tau - furthest
        half = quarters // 2
        early = tau + 1 < groups
        edge = furthest == ns - 1
        lag = tau <= groups + 1
        now = (tau > groups) & ~edge
        at_front = (z == 0) & (tau > groups) & within(gb)
        at_back = (z == ns - 1) & (tau > groups) & within(gf)
        first = jnp.where(edge | (tau < 2), tau, jnp.where(tau == 2, -1, tau - 1))
        second = jnp.where(edge | (tau < 1), tau, jnp.where(tau == 1, -1, tau - 1))
        done_f = gf - 1
        done_b = gb - 1
        done = whole - 1
        stride = parts // 4
        for p in range(parts):
            pl.when(within(gf))(lambda: chain_f(gf, p))
            pl.when(within(gb))(lambda: chain_b(gb, p))
            if (p + 1) % (parts // quarters) == 0 and p + 1 < parts:
                q = p * quarters // parts
                pl.when(at_front)(lambda: sums_b(gb, q))
                pl.when(at_back)(lambda: sums_f(gf, q))
            if p == stride - 1:
                pl.when(early)(lambda: prepare(tau + 1))
                pl.when(within(done_f) & lag & ~early)(lambda: finish_f(done_f))
            elif p == 2 * stride - 1:
                pl.when(within(first))(lambda: heavy(first, 0, half))
                pl.when(within(done_f) & early)(lambda: finish_f(done_f))
            elif p == 3 * stride - 1:
                pl.when(early)(lambda: local(tau + 1, cum_g[tau + 1], step_g[tau + 1]))
                pl.when(within(done_b) & lag)(lambda: finish_b(done_b))
                pl.when(within(done) & lag)(lambda: post(done))
            elif p == 4 * stride - 1:
                pl.when(within(second))(lambda: heavy(second, half, quarters - half))

        @pl.when(at_front)
        def _():
            sums_b(gb, quarters - 1)
            post(gb)
            results_b(gb)

        @pl.when(at_back)
        def _():
            sums_f(gf, quarters - 1)
            post(gf)
            results_f(gf)

        pl.when(now & within(gf))(lambda: finish_f(gf))
        pl.when(now & within(gb))(lambda: finish_b(gb))
        pl.when(now & within(whole))(lambda: post(whole))
        return carry

    local(0, *prepare_first(), opening=True)
    lax.fori_loop(0, groups + ns - 1, slot_step, 0)

    def product(first, count):
        raws = jnp.concatenate(
            [gathered_r[own, first * per : (first + count) * per] for own in range(nf)], axis=1
        )
        return dot(raws, gathered_x[...])

    def product_as_they_come(g):
        def term(own):
            return dot(gathered_r[own, span_of(g, per)], gathered_x[span_of(own, length)])

        total = term(f)
        for m in near_first:
            raw_copy(g, m).wait_recv()
            total = total + term(partner(m))
        return total

    own_tokens.wait()
    for m in range(1, nf):
        token_copy(m).wait_recv()
    shares = []
    for n, (first, count) in enumerate(((0, 1), (1, groups - 3), (groups - 2, 1), (groups - 1, 1))):
        place = slice(first * per, (first + count) * per)
        if first == last:
            z_recv[z, place] = product_as_they_come(last).astype(BF16)
        else:
            for g in range(first, first + count):
                for m in range(1, nf):
                    raw_copy(g, m).wait_recv()
            z_recv[z, place] = product(first, count).astype(BF16)
        copies = []
        for d in range(1, ns):
            share = z_recv.at[z, place]
            copy = pltpu.make_async_remote_copy(
                src_ref=share,
                dst_ref=share,
                send_sem=z_ssem.at[n, d - 1],
                recv_sem=z_rsem.at[n, d - 1],
                device_id={"seq": (z + d) % ns},
                device_id_type=MESH,
            )
            copy.start()
            copies.append(copy)
        shares.append((place, copies))
    for m in range(1, nf):
        token_copy(m).wait_send()
        for g in range(groups):
            weight_copy(g, m).wait_send()
            raw_copy(g, m).wait_send()

    @pl.when(z < ns - 1)
    def _():
        for g in range(groups):
            for p in range(parts):
                forward_copy(g, p).wait_send()

    @pl.when(z > 0)
    def _():
        for g in range(groups):
            for p in range(parts):
                backward_copy(g, p).wait_send()

    for place, copies in shares:
        for copy in copies:
            copy.wait_recv()
        summed = z_recv[0, place].astype(F32)
        for k in range(1, ns):
            summed = summed + z_recv[k, place].astype(F32)
        out_w[place] = summed

    for _, copies in shares:
        for copy in copies:
            copy.wait_send()


def ship(*refs):
    sems = refs[-1]
    count = len(refs) // 2
    copies = [
        pltpu.make_async_copy(refs[n], refs[count + n], sems.at[n]) for n in range(count)
    ]
    for copy in copies:
        copy.start()
    for copy in copies:
        copy.wait()


def general_kernel(
    nf,
    ns,
    tokens_hbm,
    weight_t,
    bias,
    rate_row,
    x_hbm,
    b_hbm,
    c_hbm,
    dy_hbm,
    x_out,
    b_out,
    c_out_hbm,
    out_w,
    tokens,
    x,
    b_in,
    c_out,
    dy,
    out_x,
    out_b,
    out_c,
    in_sem,
    out_sem,
    gathered,
    raw_t,
    cum_t,
    step_t,
    block_t,
    cum_g,
    step_g,
    tail_g,
    lead_g,
    state_loc,
    grad_loc,
    xs_g,
    ds_g,
    entry,
    later,
    send_f,
    send_b,
    through,
    grad_b,
    grad_c,
    col_t,
    xt_t,
    xc_t,
    ent_t,
    total,
    rs_send,
    rs_recv,
    z_recv,
    ag_ssem,
    ag_rsem,
    f_ssem,
    f_rsem,
    b_ssem,
    b_rsem,
    rs_ssem,
    rs_rsem,
    z_ssem,
    z_rsem,
):
    f = lax.axis_index("fsdp")
    z = lax.axis_index("seq")
    length = tokens.shape[0]
    heads, rows = weight_t.shape
    groups = b_in.shape[1] // STATE
    per = heads // groups
    wide = x.shape[1] // groups
    size = wide // per
    bits = nf.bit_length() - 1
    part_heads = heads // 2
    chunk = wide // 2
    loads = [
        pltpu.make_async_copy(source, target, in_sem.at[n])
        for n, (source, target) in enumerate(
            (
                (tokens_hbm, tokens),
                (x_hbm, x),
                (dy_hbm, dy),
                (b_hbm, b_in),
                (c_hbm, c_out),
            )
        )
    ]
    for load in loads:
        load.start()
    orders = (list(reversed(range(bits))), list(range(1, bits)) + [0])

    def slot_of(index, order):
        return sum(((index // 2**b) % 2) * 2**i for i, b in enumerate(order))

    def partner(j):
        return f + (1 - 2 * ((f // 2**j) % 2)) * 2**j

    barrier = pltpu.get_barrier_semaphore()
    for j in range(bits):
        pl.semaphore_signal(
            barrier, inc=1, device_id={"fsdp": partner(j)}, device_id_type=MESH
        )
    for d in range(1, ns):
        pl.semaphore_signal(
            barrier, inc=1, device_id={"seq": (z + d) % ns}, device_id_type=MESH
        )
    pl.semaphore_wait(barrier, bits + ns - 1)

    slots = [slot_of(f, order) for order in orders]
    for h in range(2):
        gathered[h, slots[h]] = weight_t[h * part_heads : (h + 1) * part_heads]
    for i in range(bits):
        copies = []
        for h in range(2):
            part = gathered.at[h, pl.ds((slots[h] // 2**i) * 2**i, 2**i)]
            copy = pltpu.make_async_remote_copy(
                src_ref=part,
                dst_ref=part,
                send_sem=ag_ssem.at[h, i],
                recv_sem=ag_rsem.at[h, i],
                device_id={"fsdp": partner(orders[h][i])},
                device_id_type=MESH,
            )
            copy.start()
            copies.append(copy)
        if i == bits - 1:
            for load in loads:
                load.wait()
        for copy in copies:
            copy.wait()

    raw = jnp.broadcast_to(bias[...], (length, heads)).T
    rate = jnp.broadcast_to(rate_row[...], (length, heads)).T
    for own in range(nf):
        weight = jnp.concatenate(
            [gathered[h, slot_of(own, orders[h])] for h in range(2)], axis=0
        )
        raw = raw + dot(weight, tokens[:, own * rows : (own + 1) * rows], 1, 1)
    step = jnp.maximum(raw, 0.0) + jnp.log1p(jnp.exp(-jnp.abs(raw)))
    before = iota((length, length), 0) <= iota((length, length), 1)
    cum = dot(-rate * step, before.astype(F32), precision=HIGH)
    raw_t[...] = raw
    cum_t[...] = cum
    step_t[...] = step
    final = cum[:, length - 1 : length]
    block_t[...] = jnp.broadcast_to(jnp.exp(final), (heads, STATE))
    both = jnp.concatenate([cum, step], axis=0).T
    cum_c = both[:, :heads]
    step_c = both[:, heads:]
    tail_c = jnp.exp(cum_c[length - 1 : length] - cum_c)
    lead_c = jnp.exp(cum_c)
    for g in range(groups):
        span = slice(g * per, (g + 1) * per)
        cum_g[g] = cum_c[:, span]
        step_g[g] = step_c[:, span]
        tail_g[g] = tail_c[:, span]
        lead_g[g] = lead_c[:, span]

    spread_one = (iota((2 * per, wide), 0) % per == iota((2 * per, wide), 1) // size).astype(BF16)
    gather_one = (iota((per, wide), 0) == iota((per, wide), 1) // size).astype(BF16)

    def expand(value):
        return dot(halves(value, 1), spread_one)

    def head_sums(value):
        high = value.astype(BF16)
        low = (value - high.astype(F32)).astype(BF16)
        return dot(gather_one, high, 1, 1) + dot(gather_one, low, 1, 1)

    def span_of(g, width):
        return pl.ds(pl.multiple_of(g * width, width), width)

    @pl.when(z == 0)
    def _():
        entry[...] = jnp.zeros_like(entry)

    @pl.when(z == ns - 1)
    def _():
        later[...] = jnp.zeros_like(later)

    spread_half = (
        iota((per, chunk), 0) % (per // 2) == iota((per, chunk), 1) // size
    ).astype(BF16)

    def piece(g):
        return g // 2, pl.ds(pl.multiple_of((g % 2) * chunk, chunk), chunk)

    def forward_copy(g):
        return pltpu.make_async_remote_copy(
            src_ref=send_f.at[piece(g)],
            dst_ref=entry.at[piece(g)],
            send_sem=f_ssem.at[g],
            recv_sem=f_rsem.at[g],
            device_id={"seq": (z + 1) % ns},
            device_id_type=MESH,
        )

    def backward_copy(g):
        return pltpu.make_async_remote_copy(
            src_ref=send_b.at[piece(g)],
            dst_ref=later.at[piece(g)],
            send_sem=b_ssem.at[g],
            recv_sem=b_rsem.at[g],
            device_id={"seq": (z + ns - 1) % ns},
            device_id_type=MESH,
        )

    def local(g):
        xs = (x[:, span_of(g, wide)].astype(F32) * expand(step_g[g] * tail_g[g])).astype(BF16)
        ds = (dy[:, span_of(g, wide)].astype(F32) * expand(lead_g[g])).astype(BF16)
        xs_g[g] = xs
        ds_g[g] = ds
        state_loc[g] = dot(xs, b_in[:, span_of(g, STATE)], 0, 0)
        grad_loc[g] = dot(ds, c_out[:, span_of(g, STATE)], 0, 0)

    def decay_rows(g):
        return dot(spread_half, halves(block_t[span_of(g, per // 2)], 0), 0, 0)

    def chain_f(g):
        @pl.when(z > 0)
        def _():
            forward_copy(g).wait_recv()

        @pl.when(z < ns - 1)
        def _():
            p = piece(g)
            send_f[p] = (decay_rows(g) * entry[p].astype(F32) + state_loc[p]).astype(BF16)
            forward_copy(g).start()

    def chain_b(g):
        @pl.when(z < ns - 1)
        def _():
            backward_copy(g).wait_recv()

        @pl.when(z > 0)
        def _():
            p = piece(g)
            send_b[p] = (decay_rows(g) * later[p].astype(F32) + grad_loc[p]).astype(BF16)
            backward_copy(g).start()

    def heavy(g):
        inputs = x[:, span_of(g, wide)]
        upstream = dy[:, span_of(g, wide)]
        b = b_in[:, span_of(g, STATE)]
        c = c_out[:, span_of(g, STATE)]
        meet = dot(b, c, 1, 1)
        upper = iota((length, length), 0) <= iota((length, length), 1)
        lanes = iota((length, 128), 1)
        cum_r = cum_t[span_of(g, per)]
        cum_l = cum_g[g]
        step_l = step_g[g]
        joint = jnp.zeros((length, length), F32)
        sums = []
        pieces = []
        for q in range(wide // 128):
            x_q = inputs[:, q * 128 : (q + 1) * 128]
            dy_q = upstream[:, q * 128 : (q + 1) * 128]
            weights = []
            masked = []
            for j in range(128 // size):
                k = q * (128 // size) + j
                mine = lanes // size == j
                pair = dot(jnp.where(mine, x_q, jnp.zeros_like(x_q)), dy_q, 1, 1)
                spread = cum_r[k : k + 1] - cum_l[:, k : k + 1]
                decay = jnp.exp(jnp.where(upper, spread, -1e30))
                weights.append((decay * meet).astype(BF16))
                masked.append(jnp.where(mine, dy_q, jnp.zeros_like(dy_q)))
                scaled = decay * pair * step_l[:, k : k + 1]
                joint = joint + scaled
                sums.append(jnp.sum(scaled * meet, axis=0, keepdims=True))
            pieces.append(
                dot(jnp.concatenate(weights, axis=1), jnp.concatenate(masked, axis=0))
            )
        passed = jnp.concatenate(pieces, axis=1)
        through[g] = passed
        col_t[span_of(g, per)] = jnp.concatenate(sums, axis=0)
        xt_t[span_of(g, per)] = head_sums(inputs.astype(F32) * passed)
        joint = joint.astype(BF16)
        grad_b[g] = dot(joint, c)
        grad_c[g] = dot(joint, b, 0, 0)

    def finish_f(g):
        c = c_out[:, span_of(g, STATE)]
        read = dot(c, entry[g], 1, 1)
        ent_t[span_of(g, per)] = head_sums(ds_g[g].astype(F32) * read)
        out_c[:, span_of(g, STATE)] = (grad_c[g] + dot(ds_g[g], entry[g])).astype(BF16)

    def finish_b(g):
        b = b_in[:, span_of(g, STATE)]
        carried = dot(b, later[g], 1, 1)
        xc_t[span_of(g, per)] = head_sums(x[:, span_of(g, wide)].astype(F32) * carried)
        inner = through[g] + expand(tail_g[g]) * carried
        out_x[:, span_of(g, wide)] = (expand(step_g[g]) * inner).astype(BF16)
        out_b[:, span_of(g, STATE)] = (grad_b[g] + dot(xs_g[g], later[g])).astype(BF16)

    def within(g):
        return jnp.logical_and(g >= 0, g < groups)

    def slot_step(tau, carry):
        gf = tau - z
        gb = tau - (ns - 1 - z)
        pl.when(tau < groups)(lambda: local(tau))
        pl.when(within(gf))(lambda: chain_f(2 * gf))
        pl.when(within(gb))(lambda: chain_b(2 * gb))
        pl.when(tau < groups)(lambda: heavy(tau))
        pl.when(within(gf))(lambda: chain_f(2 * gf + 1))
        pl.when(within(gb))(lambda: chain_b(2 * gb + 1))
        pl.when(within(gf))(lambda: finish_f(gf))
        pl.when(within(gb))(lambda: finish_b(gb))
        return carry

    lax.fori_loop(0, groups + ns - 1, slot_step, 0)
    stores = [
        pltpu.make_async_copy(source, target, out_sem.at[n])
        for n, (source, target) in enumerate(
            ((out_x, x_out), (out_b, b_out), (out_c, c_out_hbm))
        )
    ]
    for store in stores:
        store.start()

    crossing = jnp.concatenate(
        [
            dot(gather_one, (entry[g].astype(F32) * later[g].astype(F32)).astype(BF16))
            for g in range(groups)
        ],
        axis=0,
    )
    cum = cum_t[...]
    step = step_t[...]
    raw = raw_t[...]
    tail = jnp.exp(cum[:, length - 1 : length] - cum)
    xt = xt_t[...]
    tail_xc = tail * xc_t[...]
    leaving = step * tail_xc
    grad_cum = col_t[...] - step * xt + ent_t[...] - leaving
    closing = block_t[:, :1] * jnp.sum(crossing, axis=1, keepdims=True) + jnp.sum(
        leaving, axis=1, keepdims=True
    )
    after = (iota((length, length), 0) >= iota((length, length), 1)).astype(F32)
    grad_log = dot(grad_cum, after, precision=HIGH) + closing
    grad_raw = (xt + tail_xc - rate * grad_log) * jax.nn.sigmoid(raw)
    grad_raw = grad_raw.astype(BF16)

    bases = [0, 0]
    count = nf
    early = rows % 128 == 0

    def product(own, target, place, offset):
        columns = pl.ds(pl.multiple_of(own * rows, 128), rows) if early else slice(
            own * rows, (own + 1) * rows
        )
        block = dot(grad_raw, tokens[:, columns])
        for h in range(2):
            target[h, offset + place[h]] = block[
                h * part_heads : (h + 1) * part_heads
            ].astype(target.dtype)

    for j in range(bits):
        half = count // 2
        sent = pl.ds(nf - count, half)
        if j == 0 and early:
            bit = f % 2
            for i in range(half):
                place = [slot_of(2 * i, order) for order in orders]
                product(2 * i + (1 - bit), rs_send, place, 0)
        elif j == 0:
            for own in range(nf):
                product(own, total, [slot_of(own, order) for order in orders], 0)
        copies = []
        for h in range(2):
            b = orders[h][bits - 1 - j]
            bit_h = (f // 2**b) % 2
            if j > 0 or not early:
                rs_send[h, sent] = total[
                    h, pl.ds(bases[h] + (1 - bit_h) * half, half)
                ].astype(BF16)
            copy = pltpu.make_async_remote_copy(
                src_ref=rs_send.at[h, sent],
                dst_ref=rs_recv.at[h, sent],
                send_sem=rs_ssem.at[h, j],
                recv_sem=rs_rsem.at[h, j],
                device_id={"fsdp": partner(b)},
                device_id_type=MESH,
            )
            copy.start()
            copies.append(copy)
            bases[h] = bases[h] + bit_h * half
        if j == 0 and early:
            for i in range(half):
                place = [slot_of(2 * i, order) for order in orders]
                product(2 * i + bit, total, place, bit * half)
        for h in range(2):
            copies[h].wait()
            total[h, pl.ds(bases[h], half)] += rs_recv[h, sent].astype(F32)
        count = half

    z_recv[z] = jnp.concatenate([total[h, bases[h]] for h in range(2)], axis=0).astype(BF16)
    copies = []
    for d in range(1, ns):
        copy = pltpu.make_async_remote_copy(
            src_ref=z_recv.at[z],
            dst_ref=z_recv.at[z],
            send_sem=z_ssem.at[d - 1],
            recv_sem=z_rsem.at[d - 1],
            device_id={"seq": (z + d) % ns},
            device_id_type=MESH,
        )
        copy.start()
        copies.append(copy)
    for copy in copies:
        copy.wait()
    summed = z_recv[0].astype(F32)
    for k in range(1, ns):
        summed = summed + z_recv[k].astype(F32)
    out_w[...] = summed

    @pl.when(z < ns - 1)
    def _():
        for g in range(2 * groups):
            forward_copy(g).wait_send()

    @pl.when(z > 0)
    def _():
        for g in range(2 * groups):
            backward_copy(g).wait_send()

    for store in stores:
        store.wait()


def general_body(
    layer_input, dt_weight, dt_bias, decay_rate, ssm_input, in_basis, out_basis, out_cotangent
):
    nf, ns = lax.axis_size("fsdp"), lax.axis_size("seq")
    length = layer_input.shape[1]
    rows, heads = dt_weight.shape
    groups = in_basis.shape[2] // STATE
    per = heads // groups
    full = ssm_input.shape[2]
    wide = full // groups
    bits = nf.bit_length() - 1
    tall = (groups, wide, STATE)
    dma = pltpu.SemaphoreType.DMA
    v = pltpu.VMEM
    scratch = [
        v((length, layer_input.shape[2]), BF16),
        v((length, full), BF16),
        v((length, groups * STATE), BF16),
        v((length, groups * STATE), BF16),
        v((length, full), BF16),
        v((length, full), BF16),
        v((length, groups * STATE), BF16),
        v((length, groups * STATE), BF16),
        dma((5,)),
        dma((3,)),
        v((2, nf, heads // 2, rows), BF16),
        v((heads, length), F32),
        v((heads, length), F32),
        v((heads, length), F32),
        v((heads, STATE), F32),
        v((groups, length, per), F32),
        v((groups, length, per), F32),
        v((groups, length, per), F32),
        v((groups, length, per), F32),
        v(tall, F32),
        v(tall, F32),
        v((groups, length, wide), BF16),
        v((groups, length, wide), BF16),
        v(tall, BF16),
        v(tall, BF16),
        v(tall, BF16),
        v(tall, BF16),
        v((groups, length, wide), F32),
        v((groups, length, STATE), F32),
        v((groups, length, STATE), F32),
        v((heads, length), F32),
        v((heads, length), F32),
        v((heads, length), F32),
        v((heads, length), F32),
        v((2, nf, heads // 2, rows), F32),
        v((2, nf, heads // 2, rows), BF16),
        v((2, nf, heads // 2, rows), BF16),
        v((ns, heads, rows), BF16),
        dma((2, bits)),
        dma((2, bits)),
        dma((2 * groups,)),
        dma((2 * groups,)),
        dma((2 * groups,)),
        dma((2 * groups,)),
        dma((2, bits)),
        dma((2, bits)),
        dma((ns - 1,)),
        dma((ns - 1,)),
    ]
    anywhere = pl.BlockSpec(memory_space=pl.ANY)
    inside = pl.BlockSpec(memory_space=pltpu.VMEM)
    out_x, out_b, out_c, out_w = pl.pallas_call(
        functools.partial(general_kernel, nf, ns),
        out_shape=(
            jax.ShapeDtypeStruct((length, full), BF16),
            jax.ShapeDtypeStruct((length, groups * STATE), BF16),
            jax.ShapeDtypeStruct((length, groups * STATE), BF16),
            jax.ShapeDtypeStruct((heads, rows), F32),
        ),
        in_specs=[anywhere] + [inside] * 3 + [anywhere] * 4,
        out_specs=[anywhere] * 3 + [inside],
        scratch_shapes=scratch,
        compiler_params=pltpu.CompilerParams(
            collective_id=0, has_side_effects=True, vmem_limit_bytes=60 * 1024 * 1024
        ),
    )(
        layer_input[0],
        dt_weight.T,
        dt_bias[None],
        decay_rate[None],
        ssm_input[0],
        in_basis[0],
        out_basis[0],
        out_cotangent[0],
    )
    return (out_x[None], out_b[None], out_c[None], out_w.T)


def body(
    layer_input, dt_weight, dt_bias, decay_rate, ssm_input, in_basis, out_basis, out_cotangent
):
    nf, ns = lax.axis_size("fsdp"), lax.axis_size("seq")
    length = layer_input.shape[1]
    rows, heads = dt_weight.shape
    groups = in_basis.shape[2] // STATE
    per = heads // groups
    full = ssm_input.shape[2]
    wide = full // groups
    size = wide // per
    quarters = wide // QUARTER
    parts = wide // PIECE
    few = QUARTER // size
    tall = (groups, wide, STATE)
    flat = (groups, length, wide)
    dma = pltpu.SemaphoreType.DMA
    v = pltpu.VMEM
    scratch = [
        v((length, layer_input.shape[2]), BF16),
        v((1, heads), F32),
        v((1, heads), F32),
        v((length, full), BF16),
        v((length, groups * STATE), BF16),
        v((length, groups * STATE), BF16),
        v((length, full), BF16),
        dma((7,)),
        dma((2,)),
        v((nf, heads, rows), BF16),
        v((nf * length, rows), BF16),
        v((nf, heads, length), BF16),
        v((heads, length), F32),
        v((heads, length), F32),
        v((heads, length), F32),
        v((heads, length), F32),
        v((heads, length), F32),
        v((heads, STATE), F32),
        v((groups, length, per), F32),
        v((groups, length, per), F32),
        v(tall, F32),
        v((groups, length, length), F32),
        v(flat, F32),
        v(flat, F32),
        v(tall, F32),
        v(tall, F32),
        v(flat, BF16),
        v(flat, BF16),
        v(tall, BF16),
        v(tall, BF16),
        v(tall, BF16),
        v(tall, BF16),
        v(flat, F32),
        v((length, length), F32),
        v((groups, length, STATE), F32),
        v((groups, length, STATE), F32),
        v((groups, quarters, few, length), F32),
        v((groups, quarters, few, length), F32),
        v((groups, quarters, few, length), F32),
        v((groups, quarters, few, length), F32),
        v((ns, heads, rows), BF16),
        dma((groups, nf - 1)),
        dma((groups, nf - 1)),
        dma((nf - 1,)),
        dma((nf - 1,)),
        dma((groups, nf - 1)),
        dma((groups, nf - 1)),
        dma((groups, parts)),
        dma((groups, parts)),
        dma((groups, parts)),
        dma((groups, parts)),
        dma((4, ns - 1)),
        dma((4, ns - 1)),
    ]
    inside = pl.BlockSpec(memory_space=pltpu.VMEM)
    outside = pl.BlockSpec(memory_space=pltpu.HBM)
    operands = (
        layer_input[0],
        dt_weight.T,
        dt_bias[None],
        decay_rate[None],
        ssm_input[0],
        in_basis[0],
        out_basis[0],
        out_cotangent[0],
    )
    results = pl.pallas_call(
        functools.partial(kernel, nf, ns),
        out_shape=(
            jax.ShapeDtypeStruct((length, full), BF16),
            jax.ShapeDtypeStruct((length, groups * STATE), BF16),
            jax.ShapeDtypeStruct((length, groups * STATE), BF16),
            jax.ShapeDtypeStruct((heads, rows), F32),
        ),
        in_specs=[outside] * len(operands),
        out_specs=[inside] * 4,
        scratch_shapes=scratch,
        compiler_params=pltpu.CompilerParams(
            collective_id=0, has_side_effects=True, vmem_limit_bytes=40 * 1024 * 1024
        ),
    )(*[pltpu.with_memory_space_constraint(a, pltpu.HBM) for a in operands])
    anywhere = pl.BlockSpec(memory_space=pl.ANY)
    out_x, out_b, out_c, out_w = pl.pallas_call(
        ship,
        out_shape=[jax.ShapeDtypeStruct(r.shape, r.dtype) for r in results],
        in_specs=[anywhere] * 4,
        out_specs=[anywhere] * 4,
        scratch_shapes=[dma((4,))],
        compiler_params=pltpu.CompilerParams(vmem_limit_bytes=1024 * 1024),
    )(*results)
    return (out_x[None], out_b[None], out_c[None], out_w.T)


def solution(mesh):
    blocks = P("fsdp", "seq", None)
    rows = P("fsdp", None)

    def local(*args):
        nf = lax.axis_size("fsdp")
        shard = args[1].shape[0]
        lanes = args[4].shape[2] * STATE // args[5].shape[2]
        several = args[5].shape[2] // STATE > 3
        fits = several and shard % 128 == 0 and nf & (nf - 1) == 0 and lanes % (2 * QUARTER) == 0
        return (body if fits else general_body)(*args)

    return jax.shard_map(
        local,
        mesh=mesh,
        in_specs=(blocks, rows, P(), P(), blocks, blocks, blocks, blocks),
        out_specs=(blocks, blocks, blocks, rows),
        check_vma=False,
    )
```
